256 devices in a mesh: region: 16 (over z, x_hi), feat: 4 (over x_lo, core), row: 4 (over y).
Axes of the slice: x: 4 (x_hi: 2, x_lo: 2; x = x_hi * 2 + x_lo), y: 4, z: 8, core: 2. Of those that a mesh axis runs over, the one named last changes fastest.
Arguments:
- samples: bfloat16 [524288, 128], P(('region', 'row')), may hold values from -6 to 6
- targets: bfloat16 [524288, 64], P(('region', 'row')), may hold values from -6 to 6
- member: int32 [524288], P(('region', 'row')), may hold values 0 or 1
- omega: bfloat16 [128, 4096], P(None, 'feat'), may hold values from -0.5 to 0.5
- phase: float32 [4096], P('feat'), may hold values from -3.140625 to 3.140625
- factors: float32 [65536, 1024], P(('region', 'feat')), may hold values from -0.08 to 5, as said below
- weights_init: float32 [65536, 64], P(('region', 'feat'), 'row'), may hold values from -3 to 3
- duals_init: float32 [65536, 64], P(('region', 'feat'), 'row'), may hold values from -2 to 2
- consensus_init: float32 [4096, 64], P('feat', 'row'), may hold values from -3 to 3
- penalty_init: float32 [16], P('region'), may hold values from 2 to 8
Outputs:
- weights: float32 [65536, 64], P(('region', 'feat'), 'row')
- duals: float32 [65536, 64], P(('region', 'feat'), 'row')
- consensus: float32 [4096, 64], P('feat', 'row')
- penalty: float32 [16, 3], P('region')
The draws below stay inside these ranges and needn't reach their ends.
Inputs may be any that keep to these rules, and one draw needn't show every extreme that they name: factors: each 1024 x 1024 block is lower triangular, its diagonal between 3.5 and 5, its entries below the diagonal drawn independently, symmetric about zero and at most 0.08 in magnitude.
All inputs are finite; a program needn't handle non-finite values. No bound on the sum of `member` on one device may be relied on, other than what follows from the above.
Results may differ from the reference program's by a relative error of at most 0.006.
Values may be sent and summed in bfloat16 or wider, within the bound.
A program may use at most 128 MiB of HBM per device.

```python
import math
import jax
import jax.numpy as jnp
from jax import lax

INPUTS = 128
FEATURES = 4096
OUTPUTS = 64
ITERS = 3
BLOCK = 1024
REGIONS = 16
SAMPLES = 32768
N_FEAT = 4


def draw_samples(key, part):
    first_key, second_key = jax.random.split(jax.random.fold_in(key, 17))
    shape = (REGIONS * SAMPLES, INPUTS)
    values = jax.random.uniform(first_key, shape, jnp.float32, -6.0, 6.0)
    return values.astype(jnp.bfloat16)


def draw_factors(key, part):
    first_key, second_key = jax.random.split(key)
    height = REGIONS * FEATURES
    below = jnp.clip(jax.random.normal(first_key, (height, BLOCK), jnp.float32), -4.0, 4.0) * 0.02
    diagonal = jax.random.uniform(second_key, (height, 1), jnp.float32, 3.5, 5.0)
    inside = jnp.arange(height) % BLOCK
    column = jnp.arange(BLOCK)
    lower = jnp.where(column[None, :] < inside[:, None], below, 0.0)
    return lower + jnp.where(column[None, :] == inside[:, None], diagonal, 0.0)


def set_ends(result, stream_key, least, top_value):
    longest = result.shape.index(max(result.shape))
    spots = []
    for shift in (0, 1):
        where = [jax.random.randint(jax.random.fold_in(stream_key, axis), (), 0, length) for axis, length in enumerate(result.shape)]
        where[longest] = (where[longest] + shift) % result.shape[longest]
        spots.append(tuple(where))
    return result.at[spots[0]].set(least).at[spots[1]].set(top_value)


def shard_levels(stream_key, extent, pieces, low, high):
    level, own = 1.0, jax.random.fold_in(stream_key, 6)
    for dim, shards_of in pieces:
        steps = jnp.exp(jax.random.uniform(jax.random.fold_in(own, dim), (shards_of,), jnp.float32, low / len(pieces), high / len(pieces)))
        level = level * jnp.repeat(steps, extent[dim] // shards_of).reshape([-1 if axis == dim else 1 for axis in range(len(extent))])
    return level


def gaussian(key, extent, spread, limit, pieces=(), held_as=jnp.bfloat16):
    result = jax.random.normal(key, extent, jnp.float32) * spread
    if len(pieces) > 0:
        result = shard_levels(key, extent, pieces, -0.22, 0.18) * result
    return jnp.clip(result, min=-limit, max=limit).astype(held_as)


def setup_inputs(seed: int = 0) -> dict:
    key_list = jax.random.split(jax.random.key(seed), 11)
    samples = draw_samples(jax.random.fold_in(key_list[10], 71), 0)
    targets = gaussian(key_list[1], (REGIONS * SAMPLES, OUTPUTS), 1.0, 6.0, ((0, 64),))
    member = set_ends((jax.random.randint(key_list[2], (REGIONS * SAMPLES,), 0, 8) < 7).astype(jnp.int32), jax.random.fold_in(key_list[2], 1), 0, 1)
    omega = gaussian(key_list[3], (INPUTS, FEATURES), INPUTS ** -0.5, 0.5, ((1, 4),))
    phase = jnp.clip(jax.random.uniform(key_list[4], (FEATURES,), jnp.float32, -3.140625, 3.140625), -3.140625, 3.140625)
    factors = draw_factors(jax.random.fold_in(key_list[10], 71), 0)
    weights_init = gaussian(key_list[6], (REGIONS * FEATURES, OUTPUTS), 0.5, 3.0, ((0, 64), (1, 4)), jnp.float32)
    duals_init = gaussian(key_list[7], (REGIONS * FEATURES, OUTPUTS), 0.3, 2.0, ((0, 64), (1, 4)), jnp.float32)
    consensus_init = gaussian(key_list[8], (FEATURES, OUTPUTS), 0.5, 3.0, ((0, 4), (1, 4)), jnp.float32)
    penalty_init = jnp.clip(jnp.exp(math.log(8.0) - 1.3862944 * jax.random.uniform(key_list[9], (REGIONS,), jnp.float32) ** shard_levels(key_list[9], (REGIONS,), ((0, 16),), -0.2, 0.2)), 2.0, 8.0)
    return {"samples": samples, "targets": targets, "member": member, "omega": omega, "phase": phase, "factors": factors, "weights_init": weights_init, "duals_init": duals_init, "consensus_init": consensus_init, "penalty_init": penalty_init}


def features_of(inputs, omega, phase):
    angle = jnp.dot(inputs.astype(jnp.float32), omega.astype(jnp.float32), preferred_element_type=jnp.float32) + phase
    return (math.sqrt(2.0 / FEATURES) * jnp.cos(angle)).astype(jnp.bfloat16)

def block_solve(factor, right_side):
    forward = lax.linalg.triangular_solve(factor, right_side, left_side=True, lower=True)
    return lax.linalg.triangular_solve(factor, forward, left_side=True, lower=True, transpose_a=True)

def reference(samples, targets, member, omega, phase, factors, weights_init, duals_init, consensus_init, penalty_init):
    inputs = samples.reshape(REGIONS, SAMPLES, INPUTS)
    wanted = targets.reshape(REGIONS, SAMPLES, OUTPUTS)
    chosen = member.reshape(REGIONS, SAMPLES)
    blocks = factors.reshape(REGIONS, N_FEAT, BLOCK, BLOCK)
    weights = weights_init.reshape(REGIONS, FEATURES, OUTPUTS)
    duals = duals_init.reshape(REGIONS, FEATURES, OUTPUTS)
    consensus = consensus_init
    penalty = penalty_init
    offset = 0.01 * FEATURES * OUTPUTS
    history = []
    for iteration in range(ITERS):

        def region_step(items):
            region_in, region_out, region_mask, region_factor, local, dual, scalar = items
            features = features_of(region_in, omega, phase)
            predicted = jnp.dot(features.astype(jnp.float32), local.astype(jnp.bfloat16).astype(jnp.float32), preferred_element_type=jnp.float32)
            residual = (region_mask.astype(jnp.float32)[:, None] * (predicted - region_out.astype(jnp.float32))).astype(jnp.bfloat16)
            gradient = lax.dot_general(features.astype(jnp.float32), residual.astype(jnp.float32), (((0,), (0,)), ((), ())), preferred_element_type=jnp.float32)
            right_side = gradient + scalar * (local - consensus + dual)
            update = jax.vmap(block_solve)(region_factor, right_side.reshape(N_FEAT, BLOCK, OUTPUTS))
            return local - update.reshape(FEATURES, OUTPUTS)
        weights = lax.map(region_step, (inputs, wanted, chosen, blocks, weights, duals, penalty))
        scaled = penalty[:, None, None]
        updated = lax.optimization_barrier(jnp.sum(scaled * (weights + duals), axis=0)) / jnp.sum(penalty)
        duals = duals + weights - updated
        gap = lax.optimization_barrier(jnp.sum(jnp.square(weights - updated), axis=(1, 2)))
        drift = penalty * penalty * jnp.sum(jnp.square(updated - consensus))
        renewed = penalty * jnp.sqrt((gap + offset) / (drift + offset))
        duals = duals * (penalty / renewed)[:, None, None]
        consensus = updated
        penalty = renewed
        history.append(renewed)
    return (weights.reshape(REGIONS * FEATURES, OUTPUTS), duals.reshape(REGIONS * FEATURES, OUTPUTS), consensus, jnp.stack(history, axis=1))
```

```python
import functools
import math

import jax
import jax.numpy as jnp
from jax import lax
from jax.experimental import pallas as pl
from jax.experimental.pallas import tpu as pltpu
from jax.sharding import PartitionSpec as P

ITERS = 3
CORES = 2
PARTS = 2
MESH = pl.DeviceIdType.MESH
INV_TURN = 1.0 / (2.0 * math.pi)
COS_TERMS = (0.99999921, -19.73898042, 64.9286585, -85.2716283, 58.79050663, -21.07110846)
F32 = jnp.float32
BF16 = jnp.bfloat16


def dot(a, b):
    return lax.dot_general(a, b, (((1,), (0,)), ((), ())), preferred_element_type=F32)


def dot_nt(a, b):
    return lax.dot_general(a, b, (((1,), (1,)), ((), ())), preferred_element_type=F32)


def feature_tile(scale, omega, phase, samples):
    turns = dot_nt(omega, samples) * INV_TURN + phase * INV_TURN
    rest = turns - jnp.round(turns)
    square = rest * rest
    value = scale * COS_TERMS[-1]
    for term in COS_TERMS[-2::-1]:
        value = value * square + scale * term
    return value.astype(BF16)


def invert(base, factor_ref, dinv_ref, n_ref, t_ref):
    size = factor_ref.shape[0]
    t_ref[...] = jnp.zeros_like(t_ref)
    powers, totals = [], []
    for start in range(0, size, base):
        rows = factor_ref[start : start + base, :]
        row = lax.broadcasted_iota(jnp.int32, rows.shape, 0) + start
        column = lax.broadcasted_iota(jnp.int32, rows.shape, 1)
        diagonal = jnp.sum(jnp.where(row == column, rows, 0.0), axis=1, keepdims=True)
        n_ref[start : start + base, :] = jnp.where(row > column, rows / diagonal, 0.0).astype(BF16)
        block = factor_ref[start : start + base, start : start + base]
        inner_row = lax.broadcasted_iota(jnp.int32, block.shape, 0)
        inner_column = lax.broadcasted_iota(jnp.int32, block.shape, 1)
        on = jnp.sum(jnp.where(inner_row == inner_column, block, 0.0), axis=0, keepdims=True)
        dinv_ref[:, start : start + base] = 1.0 / on
        power = -n_ref[start : start + base, start : start + base].astype(F32)
        powers.append(power)
        totals.append(power)
    reach = 2
    while reach < base:
        for index in range(len(powers)):
            low = powers[index].astype(BF16)
            square = dot(low, low)
            low = square.astype(BF16)
            totals[index] = totals[index] + square + dot(totals[index].astype(BF16), low)
            powers[index] = square
        reach *= 2
    for index, start in enumerate(range(0, size, base)):
        t_ref[start : start + base, start : start + base] = totals[index].astype(BF16)
    width = base
    while width < size:
        for start in range(0, size, 2 * width):
            top = slice(start, start + width)
            bottom = slice(start + width, start + 2 * width)
            below = n_ref[bottom, top]
            first = below.astype(F32) + dot(below, t_ref[top, top])
            second = first + dot(t_ref[bottom, bottom], first.astype(BF16))
            t_ref[bottom, top] = (-second).astype(BF16)
        width *= 2


def admm_kernel(
    sizes,
    offset,
    scale,
    penalty_ref,
    samples_hbm,
    targets_hbm,
    member_hbm,
    omega_ref,
    phase_ref,
    factor_hbm,
    weights_ref,
    duals_ref,
    consensus_ref,
    out_ref,
    history_ref,
    factor_ref,
    dinv_ref,
    strict_ref,
    solve_ref,
    samples_ref,
    targets_ref,
    member_ref,
    far_omega_ref,
    far_phase_ref,
    turned_ref,
    column_ref,
    feat_ref,
    coarse_ref,
    acc_ref,
    part_ref,
    other_ref,
    resid_ref,
    gfar_ref,
    gside_ref,
    gsum_ref,
    gsend_ref,
    grow_ref,
    rs_send_ref,
    rs_recv_ref,
    mean_ref,
    gap_ref,
    load_sem,
    omega_send,
    omega_recv,
    crow_send,
    crow_recv,
    cside_send,
    cside_recv,
    core_send,
    core_recv,
    gside_send,
    gside_recv,
    grow_send,
    grow_recv,
    rs_send,
    rs_recv,
    mean_send,
    mean_recv,
    gap_send,
    gap_recv,
):
    n_region, n_feat, n_row = sizes
    narrow, width = weights_ref.shape
    outputs = n_row * narrow
    lanes = width // 128
    count = feat_ref.shape[2]
    chunk = min(1024, count)
    chunks = count // chunk
    piece_width = width // PARTS
    tile, broad = min(256, piece_width), min(512, piece_width)
    region, feat, row = lax.axis_index("region"), lax.axis_index("feat"), lax.axis_index("row")
    group = n_feat * n_row
    place = feat * n_row + row
    side = (region, lax.rem(feat + CORES, n_feat), row)
    core = (region, feat + 1 - 2 * lax.rem(feat, CORES), row)

    def row_peer(k):
        return (region, feat, lax.rem(row + k, n_row))

    def region_peer(k):
        return (lax.rem(region + k, n_region), feat, row)

    def group_peer(k):
        other = lax.rem(place + k, group)
        return (region, other // n_row, lax.rem(other, n_row))

    def remote(src, dst, send, recv, device):
        return pltpu.make_async_remote_copy(
            src_ref=src, dst_ref=dst, send_sem=send, recv_sem=recv,
            device_id=device, device_id_type=MESH,
        )

    first = pl.multiple_of((feat // CORES) * count, 128)
    span = pl.ds(first, count)
    loads = [
        pltpu.make_async_copy(samples_hbm.at[span], samples_ref, load_sem.at[0]),
        pltpu.make_async_copy(targets_hbm.at[:, span], targets_ref, load_sem.at[1]),
        pltpu.make_async_copy(member_hbm.at[:, span], member_ref, load_sem.at[2]),
        pltpu.make_async_copy(factor_hbm, factor_ref, load_sem.at[3]),
    ]
    for load in loads:
        load.start()

    barrier = pltpu.get_barrier_semaphore()
    for k in range(1, group):
        pl.semaphore_signal(barrier, inc=1, device_id=group_peer(k), device_id_type=MESH)
    for k in range(1, n_region):
        pl.semaphore_signal(barrier, inc=1, device_id=region_peer(k), device_id_type=MESH)

    trips = (width // tile) * chunks

    def prepare(omega, phase):
        turned_ref[...] = omega.astype(F32).T.astype(BF16)
        for j in range(width // tile):
            span = slice(j * tile, (j + 1) * tile)
            level = lax.broadcasted_iota(jnp.int32, (tile, tile), 0)
            across = lax.broadcasted_iota(jnp.int32, (tile, tile), 1)
            only = jnp.where(level == across, phase[:, span], 0.0)
            column_ref[span, :] = jnp.sum(only, axis=1, keepdims=True)

    def fill(half, low, high):
        def step(i, carry):
            down = pl.multiple_of((i // chunks) * tile, tile)
            right = pl.multiple_of((i % chunks) * chunk, chunk)
            feat_ref[half, pl.ds(down, tile), pl.ds(right, chunk)] = feature_tile(
                scale,
                turned_ref[pl.ds(down, tile), :],
                column_ref[pl.ds(down, tile), :],
                samples_ref[pl.ds(right, chunk), :],
            )
            return carry

        lax.fori_loop(low, high, step, 0)

    weights, duals, consensus = weights_ref[...], duals_ref[...], consensus_ref[...]
    rho = jnp.full((1, 128), penalty_ref[0], F32)
    history = jnp.zeros((1, 128), F32)
    lane = lax.broadcasted_iota(jnp.int32, (1, 128), 1)
    loads[0].wait()
    prepare(omega_ref[...], phase_ref[...])
    fill(0, 0, trips // 2)
    pl.semaphore_wait(barrier, group - 1 + n_region - 1)
    sends = []

    for t in range(ITERS):
        coarse_ref[t, 0, row] = weights.astype(BF16)
        mine = coarse_ref.at[t, 0, row]
        for k in range(1, n_row):
            copy = remote(mine, mine, crow_send.at[t, k], crow_recv.at[t, k], row_peer(k))
            copy.start()
            sends.append(copy)
        copy = remote(
            mine, coarse_ref.at[t, 1, row], cside_send.at[t, 0], cside_recv.at[t, 0], side
        )
        copy.start()
        sends.append(copy)

        if t == 0:
            exchange = [
                remote(omega_ref, far_omega_ref, omega_send.at[0], omega_recv.at[0], side),
                remote(phase_ref, far_phase_ref, omega_send.at[1], omega_recv.at[1], side),
            ]
            for copy in exchange:
                copy.start()
                sends.append(copy)
            fill(0, trips // 2, trips)

        for k in range(1, n_row):
            source = lax.rem(row - k + n_row, n_row)
            piece = coarse_ref.at[t, 0, source]
            remote(piece, piece, crow_send.at[t, k], crow_recv.at[t, k], side).wait_recv()
            copy = remote(
                piece, coarse_ref.at[t, 1, source], cside_send.at[t, k], cside_recv.at[t, k], side
            )
            copy.start()
            sends.append(copy)
        if t == 0:
            for copy in exchange:
                copy.wait_recv()
            prepare(far_omega_ref[...], far_phase_ref[...])
            fill(1, 0, trips)
            loads[1].wait()
            loads[2].wait()
        near = coarse_ref[t, 0].reshape(outputs, width)
        for j in range(chunks):
            span = slice(j * chunk, (j + 1) * chunk)
            acc_ref[:, span] = dot(near, feat_ref[0, :, span])
        for k in range(n_row):
            source = lax.rem(row - k + n_row, n_row)
            piece = coarse_ref.at[t, 1, source]
            remote(piece, piece, cside_send.at[t, k], cside_recv.at[t, k], side).wait_recv()
        far = coarse_ref[t, 1].reshape(outputs, width)
        for j in range(chunks):
            span = slice(j * chunk, (j + 1) * chunk)
            part = acc_ref[:, span] + dot(far, feat_ref[1, :, span])
            acc_ref[:, span] = part
            part_ref[t, j] = part.astype(BF16)
            copy = remote(
                part_ref.at[t, j], other_ref.at[t, j], core_send.at[t, j], core_recv.at[t, j], core
            )
            copy.start()
            sends.append(copy)
        if t > 0:
            share_mean(t - 1)
        for j in range(chunks):
            span = slice(j * chunk, (j + 1) * chunk)
            piece = other_ref.at[t, j]
            remote(piece, piece, core_send.at[t, j], core_recv.at[t, j], core).wait_recv()
            predicted = acc_ref[:, span] + other_ref[t, j].astype(F32)
            gap_value = predicted - targets_ref[:, span].astype(F32)
            resid_ref[:, span] = (member_ref[:, span].astype(F32) * gap_value).astype(BF16)

        for p in range(PARTS):
            for j in range(piece_width // broad):
                inside = slice(j * broad, (j + 1) * broad)
                span = slice(p * piece_width + j * broad, p * piece_width + (j + 1) * broad)
                value = dot_nt(resid_ref[...], feat_ref[1, span, :])
                gfar_ref[t, p, :, :, inside] = value.astype(BF16).reshape(n_row, narrow, broad)
            copy = remote(
                gfar_ref.at[t, p], gside_ref.at[t, p], gside_send.at[t, p], gside_recv.at[t, p],
                side,
            )
            copy.start()
            sends.append(copy)
        for p in range(PARTS):
            if t > 0 and p == PARTS - 1:
                duals, consensus = finish_region(t - 1)
            for j in range(piece_width // broad):
                inside = slice(j * broad, (j + 1) * broad)
                span = slice(p * piece_width + j * broad, p * piece_width + (j + 1) * broad)
                value = dot_nt(resid_ref[...], feat_ref[0, span, :])
                gsum_ref[p, :, :, inside] = value.reshape(n_row, narrow, broad)
            piece = gside_ref.at[t, p]
            remote(piece, piece, gside_send.at[t, p], gside_recv.at[t, p], side).wait_recv()
            for k in range(1, n_row):
                target = lax.rem(row + k, n_row)
                value = gsum_ref[p, target] + gside_ref[t, p, target].astype(F32)
                gsend_ref[t, p, k] = value.astype(BF16)
                copy = remote(
                    gsend_ref.at[t, p, k], grow_ref.at[t, p, k], grow_send.at[t, p, k],
                    grow_recv.at[t, p, k], row_peer(k),
                )
                copy.start()
                sends.append(copy)
        if t > 0:
            rho, duals, history = finish_gap(t - 1, rho, duals, history)
        else:
            loads[3].wait()
            invert(min(256, width), factor_ref, dinv_ref, strict_ref, solve_ref)
        dinv = dinv_ref[...]
        scalar = rho[:, :1]
        gradient = []
        for p in range(PARTS):
            value = gsum_ref[p, row] + gside_ref[t, p, row].astype(F32)
            for k in range(1, n_row):
                piece = grow_ref.at[t, p, k]
                remote(
                    piece, piece, grow_send.at[t, p, k], grow_recv.at[t, p, k], side
                ).wait_recv()
                value = value + grow_ref[t, p, k].astype(F32)
            gradient.append(value)
        right = scalar * (weights - consensus + duals) + jnp.concatenate(gradient, axis=1)
        forward = right * dinv
        forward = forward + dot_nt(forward.astype(BF16), solve_ref[...])
        backward = (forward + dot(forward.astype(BF16), solve_ref[...])) * dinv
        weights = weights - backward

        total = scalar * (weights + duals)
        for c in range(n_region):
            down, right = 8 * (c // lanes), 128 * (c % lanes)
            rs_send_ref[t, c, :8] = total[down : down + 8, right : right + 128]
            rs_send_ref[t, c, 8:] = jnp.broadcast_to(scalar, (8, 128))
        rs_recv_ref[t, region] = rs_send_ref[t, region]
        for k in range(1, n_region):
            owner = lax.rem(region + k, n_region)
            copy = remote(
                rs_send_ref.at[t, owner, pl.ds(0, 9)], rs_recv_ref.at[t, region, pl.ds(0, 9)],
                rs_send.at[t, k], rs_recv.at[t, k], region_peer(k),
            )
            copy.start()
            sends.append(copy)

        def share_mean(s):
            for k in range(1, n_region):
                source = lax.rem(region - k + n_region, n_region)
                piece = rs_recv_ref.at[s, source, pl.ds(0, 9)]
                remote(
                    piece, piece, rs_send.at[s, k], rs_recv.at[s, k], region_peer(k)
                ).wait_recv()
            total = rs_recv_ref[s, 0, :9]
            for r in range(1, n_region):
                total = total + rs_recv_ref[s, r, :9]
            mean_ref[s, region] = total[:8] / total[8:9]
            mine = mean_ref.at[s, region]
            for k in range(1, n_region):
                copy = remote(mine, mine, mean_send.at[s, k], mean_recv.at[s, k], region_peer(k))
                copy.start()
                sends.append(copy)

        def finish_region(s, weights=weights, duals=duals, consensus=consensus):
            for k in range(1, n_region):
                source = lax.rem(region - k + n_region, n_region)
                piece = mean_ref.at[s, source]
                remote(
                    piece, piece, mean_send.at[s, k], mean_recv.at[s, k], region_peer(k)
                ).wait_recv()
            updated = jnp.concatenate(
                [
                    jnp.concatenate([mean_ref[s, h * lanes + j] for j in range(lanes)], axis=1)
                    for h in range(narrow // 8)
                ],
                axis=0,
            )
            gap = jnp.sum(jnp.square(weights - updated), keepdims=True).reshape(1, 1)
            drift = jnp.sum(jnp.square(updated - consensus), keepdims=True).reshape(1, 1)
            level = lax.broadcasted_iota(jnp.int32, (8, 128), 0)
            gap_ref[s, place] = jnp.where(level == 0, gap, drift)
            mine = gap_ref.at[s, place]
            for k in range(1, group):
                copy = remote(mine, mine, gap_send.at[s, k], gap_recv.at[s, k], group_peer(k))
                copy.start()
                sends.append(copy)
            return duals + weights - updated, updated

        def finish_gap(s, rho, duals, history):
            for k in range(1, group):
                source = lax.rem(place - k + group, group)
                piece = gap_ref.at[s, source]
                remote(
                    piece, piece, gap_send.at[s, k], gap_recv.at[s, k], group_peer(k)
                ).wait_recv()
            total = jnp.sum(gap_ref[s], axis=0)
            gap, drift = total[0:1], total[1:2]
            drift = rho * rho * drift
            renewed = rho * jnp.sqrt((gap + offset) / (drift + offset))
            duals = duals * (rho / renewed)[:, :1]
            return renewed, duals, jnp.where(lane == s, renewed, history)

    share_mean(ITERS - 1)
    duals, consensus = finish_region(ITERS - 1)
    rho, duals, history = finish_gap(ITERS - 1, rho, duals, history)
    out_ref[0] = weights
    out_ref[1] = duals
    out_ref[2] = consensus
    history_ref[...] = history
    for copy in sends:
        copy.wait_send()


def admm(sizes, offset, scale, penalty, samples, targets, member, omega, phase, factors, *state):
    n_region, n_feat, n_row = sizes
    narrow, width = state[0].shape
    outputs = n_row * narrow
    inputs = omega.shape[0]
    count = samples.shape[0] // (n_feat // CORES)
    chunk = min(1024, count)
    chunks = count // chunk
    group = n_feat * n_row
    part = (n_row, narrow, width // PARTS)
    vmem = pl.BlockSpec(memory_space=pltpu.VMEM)
    hbm = pl.BlockSpec(memory_space=pl.ANY)
    dma = pltpu.SemaphoreType.DMA
    return pl.pallas_call(
        functools.partial(admm_kernel, sizes, offset, scale),
        in_specs=[pl.BlockSpec(memory_space=pltpu.SMEM), hbm, hbm, hbm] + [vmem, vmem, hbm, vmem, vmem, vmem],
        out_specs=[vmem, vmem],
        out_shape=[
            jax.ShapeDtypeStruct((3, narrow, width), F32),
            jax.ShapeDtypeStruct((1, 128), F32),
        ],
        scratch_shapes=[
            pltpu.VMEM((width, width), F32),
            pltpu.VMEM((1, width), F32),
            pltpu.VMEM((width, width), BF16),
            pltpu.VMEM((width, width), BF16),
            pltpu.VMEM((count, inputs), BF16),
            pltpu.VMEM((outputs, count), BF16),
            pltpu.VMEM((1, count), jnp.int32),
            pltpu.VMEM((inputs, width), BF16),
            pltpu.VMEM((1, width), F32),
            pltpu.VMEM((width, inputs), BF16),
            pltpu.VMEM((width, 1), F32),
            pltpu.VMEM((2, width, count), BF16),
            pltpu.VMEM((ITERS, 2, n_row, narrow, width), BF16),
            pltpu.VMEM((outputs, count), F32),
            pltpu.VMEM((ITERS, chunks, outputs, chunk), BF16),
            pltpu.VMEM((ITERS, chunks, outputs, chunk), BF16),
            pltpu.VMEM((outputs, count), BF16),
            pltpu.VMEM((ITERS, PARTS) + part, BF16),
            pltpu.VMEM((ITERS, PARTS) + part, BF16),
            pltpu.VMEM((PARTS,) + part, F32),
            pltpu.VMEM((ITERS, PARTS) + part, BF16),
            pltpu.VMEM((ITERS, PARTS) + part, BF16),
            pltpu.VMEM((ITERS, n_region, 16, 128), F32),
            pltpu.VMEM((ITERS, n_region, 16, 128), F32),
            pltpu.VMEM((ITERS, n_region, 8, 128), F32),
            pltpu.VMEM((ITERS, group, 8, 128), F32),
            dma((4,)),
            dma((2,)),
            dma((2,)),
            dma((ITERS, n_row)),
            dma((ITERS, n_row)),
            dma((ITERS, n_row)),
            dma((ITERS, n_row)),
            dma((ITERS, chunks)),
            dma((ITERS, chunks)),
            dma((ITERS, PARTS)),
            dma((ITERS, PARTS)),
            dma((ITERS, PARTS, n_row)),
            dma((ITERS, PARTS, n_row)),
            dma((ITERS, n_region)),
            dma((ITERS, n_region)),
            dma((ITERS, n_region)),
            dma((ITERS, n_region)),
            dma((ITERS, group)),
            dma((ITERS, group)),
        ],
        compiler_params=pltpu.CompilerParams(
            collective_id=0, has_side_effects=True, vmem_limit_bytes=56 * 2**20
        ),
        name="admm",
    )(penalty, samples, targets, member, omega, phase, factors, *state)


def per_device(
    sizes,
    samples,
    targets,
    member,
    omega,
    phase,
    factors,
    weights_init,
    duals_init,
    consensus_init,
    penalty_init,
):
    n_region, n_feat, n_row = sizes
    total_features = n_feat * omega.shape[1]
    total_outputs = targets.shape[1]
    offset = 0.01 * total_features * total_outputs
    scale = math.sqrt(2.0 / total_features)
    final, history = admm(
        sizes, offset, scale, penalty_init, samples, targets.T, member[None, :], omega,
        phase[None, :], factors, weights_init.T, duals_init.T, consensus_init.T,
    )
    return (final[0].T, final[1].T, final[2].T, history[:, :ITERS])


def solution(mesh):
    sizes = (mesh.shape["region"], mesh.shape["feat"], mesh.shape["row"])
    return jax.shard_map(
        functools.partial(per_device, sizes),
        mesh=mesh,
        in_specs=(
            P(("region", "row"), None),
            P(("region", "row"), None),
            P(("region", "row")),
            P(None, "feat"),
            P("feat"),
            P(("region", "feat"), None),
            P(("region", "feat"), "row"),
            P(("region", "feat"), "row"),
            P("feat", "row"),
            P("region"),
        ),
        out_specs=(
            P(("region", "feat"), "row"),
            P(("region", "feat"), "row"),
            P("feat", "row"),
            P("region", None),
        ),
        check_vma=False,
    )
```

```python
import functools
import math

import jax
import jax.numpy as jnp
from jax import lax
from jax.experimental import pallas as pl
from jax.experimental.pallas import tpu as pltpu
from jax.sharding import PartitionSpec as P

ITERS = 3
CORES = 2
PARTS = 2
CHUNK = 2048
MESH = pl.DeviceIdType.MESH
INV_TURN = 1.0 / (2.0 * math.pi)
WAVE_GAIN, WAVE_MIDDLE, WAVE_LAST = 71.848585, -0.5703125, 0.08740234375
F32 = jnp.float32
BF16 = jnp.bfloat16


def dot(a, b):
    return lax.dot_general(a, b, (((1,), (0,)), ((), ())), preferred_element_type=F32)


def dot_nt(a, b):
    return lax.dot_general(a, b, (((1,), (1,)), ((), ())), preferred_element_type=F32)


def feature_tile(omega, phase, samples):
    turns = dot_nt(omega, samples) + phase
    rest = (0.25 - jnp.abs(turns - jnp.round(turns))).astype(BF16)
    square = rest * rest
    value = (square + jnp.asarray(WAVE_MIDDLE, BF16)) * square + jnp.asarray(WAVE_LAST, BF16)
    return value * rest


def invert(base, factor_ref, dinv_ref, n_ref, t_ref):
    size = factor_ref.shape[0]
    t_ref[...] = jnp.zeros_like(t_ref)
    powers, totals = [], []
    for start in range(0, size, base):
        rows = factor_ref[start : start + base, :]
        row = lax.broadcasted_iota(jnp.int32, rows.shape, 0) + start
        column = lax.broadcasted_iota(jnp.int32, rows.shape, 1)
        diagonal = jnp.sum(jnp.where(row == column, rows, 0.0), axis=1, keepdims=True)
        n_ref[start : start + base, :] = jnp.where(row > column, rows / diagonal, 0.0).astype(BF16)
        block = factor_ref[start : start + base, start : start + base]
        inner_row = lax.broadcasted_iota(jnp.int32, block.shape, 0)
        inner_column = lax.broadcasted_iota(jnp.int32, block.shape, 1)
        on = jnp.sum(jnp.where(inner_row == inner_column, block, 0.0), axis=0, keepdims=True)
        dinv_ref[:, start : start + base] = 1.0 / on
        power = -n_ref[start : start + base, start : start + base].astype(F32)
        powers.append(power)
        totals.append(power)
    reach = 2
    while reach < base:
        for index in range(len(powers)):
            low = powers[index].astype(BF16)
            square = dot(low, low)
            low = square.astype(BF16)
            totals[index] = totals[index] + square + dot(totals[index].astype(BF16), low)
            powers[index] = square
        reach *= 2
    for index, start in enumerate(range(0, size, base)):
        t_ref[start : start + base, start : start + base] = totals[index].astype(BF16)
    width = base
    while width < size:
        for start in range(0, size, 2 * width):
            top = slice(start, start + width)
            bottom = slice(start + width, start + 2 * width)
            below = n_ref[bottom, top]
            first = below.astype(F32) + dot(below, t_ref[top, top])
            second = first + dot(t_ref[bottom, bottom], first.astype(BF16))
            t_ref[bottom, top] = (-second).astype(BF16)
        width *= 2


def admm_kernel(
    sizes,
    offset,
    scale,
    penalty_ref,
    samples_hbm,
    targets_hbm,
    member_hbm,
    omega_hbm,
    phase_hbm,
    factor_hbm,
    weights_hbm,
    duals_hbm,
    consensus_hbm,
    out_hbm,
    factor_ref,
    dinv_ref,
    strict_ref,
    solve_ref,
    samples_ref,
    targets_ref,
    member_ref,
    omega_ref,
    phase_ref,
    state_ref,
    feat_ref,
    flip_ref,
    coarse_ref,
    acc_ref,
    part_ref,
    other_ref,
    resid_ref,
    gfar_ref,
    gside_ref,
    gown_ref,
    gsend_ref,
    grow_ref,
    rs_send_ref,
    rs_recv_ref,
    mean_ref,
    gap_ref,
    load_sem,
    store_sem,
    omega_send,
    omega_recv,
    phase_send,
    phase_recv,
    crow_send,
    crow_recv,
    cside_send,
    cside_recv,
    core_send,
    core_recv,
    gside_send,
    gside_recv,
    grow_send,
    grow_recv,
    rs_send,
    rs_recv,
    mean_send,
    mean_recv,
    gap_send,
    gap_recv,
):
    n_region, n_feat, n_row = sizes
    narrow, width = weights_hbm.shape
    outputs = n_row * narrow
    lanes = width // 128
    inputs = omega_hbm.shape[0]
    gain = scale * WAVE_GAIN
    count = feat_ref.shape[2]
    chunk = min(CHUNK, count)
    chunks = count // chunk
    piece_width = width // PARTS
    tile = min(512, piece_width)
    tiles = width // tile
    region, feat, row = lax.axis_index("region"), lax.axis_index("feat"), lax.axis_index("row")
    group = n_feat * n_row
    place = feat * n_row + row
    side = (region, lax.rem(feat + CORES, n_feat), row)
    core = (region, feat + 1 - 2 * lax.rem(feat, CORES), row)

    def row_peer(k):
        return (region, feat, lax.rem(row + k, n_row))

    def region_peer(k):
        return (lax.rem(region + k, n_region), feat, row)

    def far_peer(k):
        return (region, lax.rem(feat + CORES, n_feat), lax.rem(row + k, n_row))

    def group_peer(k):
        other = lax.rem(place + k, group)
        return (region, other // n_row, lax.rem(other, n_row))

    def remote(src, dst, send, recv, device):
        return pltpu.make_async_remote_copy(
            src_ref=src, dst_ref=dst, send_sem=send, recv_sem=recv,
            device_id=device, device_id_type=MESH,
        )

    first = pl.multiple_of((feat // CORES) * count, 128)
    span = pl.ds(first, count)
    loads = [
        pltpu.make_async_copy(samples_hbm.at[span], samples_ref.at[:, :inputs], load_sem.at[0]),
        pltpu.make_async_copy(omega_hbm, omega_ref.at[0], load_sem.at[1]),
        pltpu.make_async_copy(phase_hbm, phase_ref.at[0], load_sem.at[2]),
        pltpu.make_async_copy(weights_hbm, state_ref.at[0], load_sem.at[3]),
        pltpu.make_async_copy(duals_hbm, state_ref.at[1], load_sem.at[4]),
        pltpu.make_async_copy(consensus_hbm, state_ref.at[2], load_sem.at[5]),
        pltpu.make_async_copy(targets_hbm.at[:, span], targets_ref, load_sem.at[6]),
        pltpu.make_async_copy(member_hbm.at[:, span], member_ref, load_sem.at[7]),
        pltpu.make_async_copy(factor_hbm, factor_ref, load_sem.at[8]),
    ]
    for load in loads[:6]:
        load.start()

    barrier = pltpu.get_barrier_semaphore()
    for k in range(1, group):
        pl.semaphore_signal(barrier, inc=1, device_id=group_peer(k), device_id_type=MESH)
    for k in range(1, n_region):
        pl.semaphore_signal(barrier, inc=1, device_id=region_peer(k), device_id_type=MESH)

    def column_of(line):
        pieces = []
        for j in range(tile // 128):
            level = lax.broadcasted_iota(jnp.int32, (128, 128), 0)
            across = lax.broadcasted_iota(jnp.int32, (128, 128), 1)
            only = jnp.where(level == across, line[:, 128 * j : 128 * (j + 1)], 0.0)
            pieces.append(jnp.sum(only, axis=1, keepdims=True))
        return jnp.concatenate(pieces, axis=0)

    def omega_piece(i):
        span = pl.ds(pl.multiple_of(i * tile, tile), tile)
        return remote(
            omega_ref.at[0, :, span], omega_ref.at[1, :, span], omega_send.at[i], omega_recv.at[i],
            side,
        )

    def phase_copy():
        return remote(phase_ref.at[0], phase_ref.at[1], phase_send.at[0], phase_recv.at[0], side)

    def near_copies(t):
        mine = coarse_ref.at[t, 0, row]
        return [
            remote(mine, mine, crow_send.at[t], crow_recv.at[t], row_peer(k))
            for k in range(1, n_row)
        ]

    def far_copies(t):
        mine, there = coarse_ref.at[t, 0, row], coarse_ref.at[t, 1, row]
        return [
            remote(mine, there, cside_send.at[t], cside_recv.at[t], far_peer(k))
            for k in range(n_row)
        ]

    def arrived(pieces, semaphore):
        remote(pieces, pieces, semaphore, semaphore, side).wait_recv()

    def sent(pieces, semaphore):
        remote(pieces, pieces, semaphore, semaphore, side).wait_send()

    def core_copy(t, j):
        return remote(
            part_ref.at[t, j], other_ref.at[t, j], core_send.at[t, j], core_recv.at[t, j], core
        )

    def start(copies):
        for copy in copies:
            copy.start()

    def fill(i, carry):
        half, piece = i // tiles, lax.rem(i, tiles)

        @pl.when(i == 1)
        def _():
            pl.semaphore_wait(barrier, group - 1 + n_region - 1)
            start([phase_copy()])
            start([omega_piece(j) for j in range(tiles)])
            coarse_ref[0, 0, row] = state_ref[0].astype(BF16)
            start(near_copies(0))
            start(far_copies(0))

        @pl.when(i == tiles)
        def _():
            phase_copy().wait_recv()

        @pl.when(i >= tiles)
        def _():
            omega_piece(piece).wait_recv()

        down = pl.multiple_of(piece * tile, tile)
        part = (omega_ref[half, :, pl.ds(down, tile)].astype(F32) * INV_TURN).T
        high = part.astype(BF16)
        low = (part - high.astype(F32)).astype(BF16)
        column = column_of(phase_ref[half, :, pl.ds(down, tile)] * INV_TURN)
        both = jnp.concatenate([high, low], axis=1)
        value = feature_tile(both, column, samples_ref[...])
        feat_ref[half, pl.ds(down, tile), :] = value
        flip_ref[half, :, pl.ds(down, tile)] = value.T
        return carry

    rho = jnp.full((1, 128), penalty_ref[0], F32)
    history = jnp.zeros((1, 128), F32)
    lane = lax.broadcasted_iota(jnp.int32, (1, 128), 1)
    with jax.named_scope("load0"):
        for load in loads[:6]:
            load.wait()
        for load in loads[6:]:
            load.start()
        samples_ref[:, inputs:] = samples_ref[:, :inputs]
    with jax.named_scope("fill"):
        lax.fori_loop(0, 2 * tiles, fill, 0)
    weights, duals, consensus = state_ref[0], state_ref[1], state_ref[2]

    for t in range(ITERS):
        with jax.named_scope("near_wait"):
            arrived(coarse_ref.at[t, 0, pl.ds(0, n_row - 1)], crow_recv.at[t])
        if t == 0:
            loads[6].wait()
            loads[7].wait()
        with jax.named_scope("pred_near"):
            near = coarse_ref[t, 0].reshape(outputs, width)
            for j in range(chunks):
                span = slice(j * chunk, (j + 1) * chunk)
                acc_ref[:, span] = dot(near, feat_ref[0, :, span])
        with jax.named_scope("far_wait"):
            arrived(coarse_ref.at[t, 1], cside_recv.at[t])
        with jax.named_scope("pred_far"):
            far = coarse_ref[t, 1].reshape(outputs, width)
            for j in range(chunks):
                if t > 0 and j == chunks - 1:
                    with jax.named_scope("share_mean"):
                        share_mean(t - 1)
                span = slice(j * chunk, (j + 1) * chunk)
                part = gain * (acc_ref[:, span] + dot(far, feat_ref[1, :, span]))
                acc_ref[:, span] = part
                part_ref[t, j] = part.astype(BF16)
                core_copy(t, j).start()
        with jax.named_scope("resid"):
            for j in range(chunks):
                span = slice(j * chunk, (j + 1) * chunk)
                core_copy(t, j).wait_recv()
                predicted = acc_ref[:, span] + other_ref[t, j].astype(F32)
                gap_value = predicted - targets_ref[:, span].astype(F32)
                resid_ref[:, span] = (member_ref[:, span].astype(F32) * gap_value).astype(BF16)

        with jax.named_scope("grad_far"):
            for p in range(PARTS):
                span = slice(p * piece_width, (p + 1) * piece_width)
                value = dot(resid_ref[...], flip_ref[1, :, span])
                gfar_ref[t, p] = value.astype(BF16).reshape(n_row, narrow, piece_width)
                for k in range(n_row):
                    target = lax.rem(row + k, n_row)
                    copy = remote(
                        gfar_ref.at[t, p, target], gside_ref.at[t, p, k], gside_send.at[t],
                        gside_recv.at[t], far_peer(k),
                    )
                    copy.start()
        with jax.named_scope("grad_near"):
            for p in range(PARTS):
                span = slice(p * piece_width, (p + 1) * piece_width)
                value = dot(resid_ref[...], flip_ref[0, :, span])
                value = value.reshape(n_row, narrow, piece_width)
                gown_ref[p] = value
                gsend_ref[t, p] = value.astype(BF16)
                for k in range(1, n_row):
                    target = lax.rem(row + k, n_row)
                    copy = remote(
                        gsend_ref.at[t, p, target], grow_ref.at[t, p, k], grow_send.at[t],
                        grow_recv.at[t], row_peer(k),
                    )
                    copy.start()
        if t == 0:
            with jax.named_scope("invert"):
                loads[8].wait()
                invert(min(256, width), factor_ref, dinv_ref, strict_ref, solve_ref)
        else:
            with jax.named_scope("finish_region"):
                apart, duals, consensus = finish_region(t - 1)
        dinv = dinv_ref[...]
        with jax.named_scope("grad_wait"):
            arrived(gside_ref.at[t], gside_recv.at[t])
            arrived(grow_ref.at[t, :, pl.ds(1, n_row - 1)], grow_recv.at[t])
            gradient = []
            for p in range(PARTS):
                value = gown_ref[p, row]
                for k in range(n_row):
                    value = value + gside_ref[t, p, k].astype(F32)
                for k in range(1, n_row):
                    value = value + grow_ref[t, p, k].astype(F32)
                gradient.append(value)
            gradient = gain * jnp.concatenate(gradient, axis=1)
        with jax.named_scope("solve"):
            scalar = rho[:, :1]
            if t == 0:
                right = gradient + scalar * (weights - consensus + duals)
            else:
                right = jnp.concatenate([gradient + scalar * duals, apart], axis=0)
            forward = right * dinv
            forward = forward + dot_nt(forward.astype(BF16), solve_ref[...])
            update = (forward + dot(forward.astype(BF16), solve_ref[...])) * dinv
        if t > 0:
            with jax.named_scope("finish_gap"):
                rho, duals, history = finish_gap(t - 1, rho, duals, history)
            scalar = rho[:, :1]
            update = update[:narrow] + scalar * update[narrow:]
        weights = weights - update
        if t < ITERS - 1:
            coarse_ref[t + 1, 0, row] = weights.astype(BF16)
            start(near_copies(t + 1))

        total = scalar * (weights + duals)
        for c in range(n_region):
            down, right = 8 * (c // lanes), 128 * (c % lanes)
            rs_send_ref[t, c, :8] = total[down : down + 8, right : right + 128]
            rs_send_ref[t, c, 8:] = jnp.broadcast_to(scalar, (8, 128))
        rs_recv_ref[t, region] = rs_send_ref[t, region]
        for k in range(1, n_region):
            owner = lax.rem(region + k, n_region)
            copy = remote(
                rs_send_ref.at[t, owner, pl.ds(0, 9)], rs_recv_ref.at[t, region, pl.ds(0, 9)],
                rs_send.at[t], rs_recv.at[t], region_peer(k),
            )
            copy.start()
        if t < ITERS - 1:
            start(far_copies(t + 1))

        def share_mean(s):
            arrived(rs_recv_ref.at[s, pl.ds(0, n_region - 1), pl.ds(0, 9)], rs_recv.at[s])
            total = rs_recv_ref[s, 0, :9]
            for r in range(1, n_region):
                total = total + rs_recv_ref[s, r, :9]
            mean_ref[s, region] = total[:8] / total[8:9]
            mine = mean_ref.at[s, region]
            for k in range(1, n_region):
                remote(mine, mine, mean_send.at[s], mean_recv.at[s], region_peer(k)).start()

        def finish_region(s, weights=weights, duals=duals, consensus=consensus):
            arrived(mean_ref.at[s, pl.ds(0, n_region - 1)], mean_recv.at[s])
            updated = jnp.concatenate(
                [
                    jnp.concatenate([mean_ref[s, h * lanes + j] for j in range(lanes)], axis=1)
                    for h in range(narrow // 8)
                ],
                axis=0,
            )
            gap = jnp.sum(jnp.square(weights - updated), keepdims=True).reshape(1, 1)
            drift = jnp.sum(jnp.square(updated - consensus), keepdims=True).reshape(1, 1)
            level = lax.broadcasted_iota(jnp.int32, (8, 128), 0)
            gap_ref[s, place] = jnp.where(level == 0, gap, drift)
            mine = gap_ref.at[s, place]
            for k in range(1, group):
                remote(mine, mine, gap_send.at[s], gap_recv.at[s], group_peer(k)).start()
            return weights - updated, duals + weights - updated, updated

        def finish_gap(s, rho, duals, history):
            arrived(gap_ref.at[s, pl.ds(0, group - 1)], gap_recv.at[s])
            total = jnp.sum(gap_ref[s], axis=0)
            gap, drift = total[0:1], total[1:2]
            drift = rho * rho * drift
            renewed = rho * jnp.sqrt((gap + offset) / (drift + offset))
            duals = duals * (rho / renewed)[:, :1]
            return renewed, duals, jnp.where(lane == s, renewed, history)

    def store(rows, value):
        state_ref[rows] = value
        copy = pltpu.make_async_copy(state_ref.at[rows], out_hbm.at[rows], store_sem.at[rows])
        copy.start()
        return copy

    stores = [store(0, weights)]
    with jax.named_scope("last_mean"):
        share_mean(ITERS - 1)
    with jax.named_scope("last_region"):
        apart, duals, consensus = finish_region(ITERS - 1)
    stores.append(store(2, consensus))
    with jax.named_scope("last_gap"):
        rho, duals, history = finish_gap(ITERS - 1, rho, duals, history)
    stores.append(store(1, duals))
    stores.append(store(3, jnp.broadcast_to(jnp.tile(history, (1, width // 128)), (narrow, width))))
    with jax.named_scope("drain"):
        phase_copy().wait_send()
        for i in range(tiles):
            omega_piece(i).wait_send()
        for t in range(ITERS):
            sent(coarse_ref.at[t, 0, pl.ds(0, n_row - 1)], crow_send.at[t])
            sent(coarse_ref.at[t, 1], cside_send.at[t])
            for j in range(chunks):
                core_copy(t, j).wait_send()
            sent(gside_ref.at[t], gside_send.at[t])
            sent(grow_ref.at[t, :, pl.ds(1, n_row - 1)], grow_send.at[t])
            sent(rs_recv_ref.at[t, pl.ds(0, n_region - 1), pl.ds(0, 9)], rs_send.at[t])
            sent(mean_ref.at[t, pl.ds(0, n_region - 1)], mean_send.at[t])
            sent(gap_ref.at[t, pl.ds(0, group - 1)], gap_send.at[t])
        for copy in stores:
            copy.wait()


def admm(sizes, offset, scale, penalty, samples, targets, member, omega, phase, factors, *state):
    n_region, n_feat, n_row = sizes
    narrow, width = state[0].shape
    outputs = n_row * narrow
    inputs = omega.shape[0]
    count = samples.shape[0] // (n_feat // CORES)
    chunk = min(CHUNK, count)
    chunks = count // chunk
    group = n_feat * n_row
    part = (n_row, narrow, width // PARTS)
    tiles = width // min(512, width // PARTS)
    hbm = pl.BlockSpec(memory_space=pl.ANY)
    dma = pltpu.SemaphoreType.DMA
    return pl.pallas_call(
        functools.partial(admm_kernel, sizes, offset, scale),
        in_specs=[pl.BlockSpec(memory_space=pltpu.SMEM)] + [hbm] * 9,
        out_specs=hbm,
        out_shape=jax.ShapeDtypeStruct((4, narrow, width), F32),
        scratch_shapes=[
            pltpu.VMEM((width, width), F32),
            pltpu.VMEM((1, width), F32),
            pltpu.VMEM((width, width), BF16),
            pltpu.VMEM((width, width), BF16),
            pltpu.VMEM((count, 2 * inputs), BF16),
            pltpu.VMEM((outputs, count), BF16),
            pltpu.VMEM((1, count), jnp.int32),
            pltpu.VMEM((2, inputs, width), BF16),
            pltpu.VMEM((2, 1, width), F32),
            pltpu.VMEM((4, narrow, width), F32),
            pltpu.VMEM((2, width, count), BF16),
            pltpu.VMEM((2, count, width), BF16),
            pltpu.VMEM((ITERS, 2, n_row, narrow, width), BF16),
            pltpu.VMEM((outputs, count), F32),
            pltpu.VMEM((ITERS, chunks, outputs, chunk), BF16),
            pltpu.VMEM((ITERS, chunks, outputs, chunk), BF16),
            pltpu.VMEM((outputs, count), BF16),
            pltpu.VMEM((ITERS, PARTS) + part, BF16),
            pltpu.VMEM((ITERS, PARTS) + part, BF16),
            pltpu.VMEM((PARTS,) + part, F32),
            pltpu.VMEM((ITERS, PARTS) + part, BF16),
            pltpu.VMEM((ITERS, PARTS) + part, BF16),
            pltpu.VMEM((ITERS, n_region, 16, 128), F32),
            pltpu.VMEM((ITERS, n_region, 16, 128), F32),
            pltpu.VMEM((ITERS, n_region, 8, 128), F32),
            pltpu.VMEM((ITERS, group, 8, 128), F32),
            dma((9,)),
            dma((4,)),
            dma((tiles,)),
            dma((tiles,)),
            dma((1,)),
            dma((1,)),
            dma((ITERS,)),
            dma((ITERS,)),
            dma((ITERS,)),
            dma((ITERS,)),
            dma((ITERS, chunks)),
            dma((ITERS, chunks)),
            dma((ITERS,)),
            dma((ITERS,)),
            dma((ITERS,)),
            dma((ITERS,)),
            dma((ITERS,)),
            dma((ITERS,)),
            dma((ITERS,)),
            dma((ITERS,)),
            dma((ITERS,)),
            dma((ITERS,)),
        ],
        compiler_params=pltpu.CompilerParams(
            collective_id=0, has_side_effects=True, vmem_limit_bytes=63 * 2**20
        ),
        name="admm",
    )(penalty, samples, targets, member, omega, phase, factors, *state)


def per_device(
    sizes,
    samples,
    targets,
    member,
    omega,
    phase,
    factors,
    weights_init,
    duals_init,
    consensus_init,
    penalty_init,
):
    n_region, n_feat, n_row = sizes
    total_features = n_feat * omega.shape[1]
    total_outputs = targets.shape[1]
    offset = 0.01 * total_features * total_outputs
    scale = math.sqrt(2.0 / total_features)
    final = admm(
        sizes, offset, scale, penalty_init, samples, targets.T, member[None, :], omega,
        phase[None, :], factors, weights_init.T, duals_init.T, consensus_init.T,
    )
    return (final[0].T, final[1].T, final[2].T, final[3, :1, :ITERS])


def solution(mesh):
    sizes = (mesh.shape["region"], mesh.shape["feat"], mesh.shape["row"])
    return jax.shard_map(
        functools.partial(per_device, sizes),
        mesh=mesh,
        in_specs=(
            P(("region", "row"), None),
            P(("region", "row"), None),
            P(("region", "row")),
            P(None, "feat"),
            P("feat"),
            P(("region", "feat"), None),
            P(("region", "feat"), "row"),
            P(("region", "feat"), "row"),
            P("feat", "row"),
            P("region"),
        ),
        out_specs=(
            P(("region", "feat"), "row"),
            P(("region", "feat"), "row"),
            P("feat", "row"),
            P("region", None),
        ),
        check_vma=False,
    )
```

```python
import functools
import math

import jax
import jax.numpy as jnp
from jax import lax
from jax.experimental import pallas as pl
from jax.experimental.pallas import tpu as pltpu
from jax.sharding import PartitionSpec as P

ITERS = 3
CORES = 2
PARTS = 2
CHUNK = 2048
MESH = pl.DeviceIdType.MESH
INV_TURN = 1.0 / (2.0 * math.pi)
WAVE_GAIN, WAVE_MIDDLE, WAVE_LAST = 71.848585, -0.5703125, 0.08740234375
F32 = jnp.float32
BF16 = jnp.bfloat16


def dot(a, b):
    return lax.dot_general(a, b, (((1,), (0,)), ((), ())), preferred_element_type=F32)


def dot_nt(a, b):
    return lax.dot_general(a, b, (((1,), (1,)), ((), ())), preferred_element_type=F32)


def feature_tile(omega, phase, samples):
    turns = dot_nt(omega, samples) + phase
    rest = (0.25 - jnp.abs(turns - jnp.round(turns))).astype(BF16)
    square = rest * rest
    value = (square + jnp.asarray(WAVE_MIDDLE, BF16)) * square + jnp.asarray(WAVE_LAST, BF16)
    return value * rest


def invert(base, factor_ref, dinv_ref, n_ref, t_ref):
    size = factor_ref.shape[0]
    t_ref[...] = jnp.zeros_like(t_ref)
    powers, totals = [], []
    for start in range(0, size, base):
        rows = factor_ref[start : start + base, :]
        row = lax.broadcasted_iota(jnp.int32, rows.shape, 0) + start
        column = lax.broadcasted_iota(jnp.int32, rows.shape, 1)
        diagonal = jnp.sum(jnp.where(row == column, rows, 0.0), axis=1, keepdims=True)
        n_ref[start : start + base, :] = jnp.where(row > column, rows / diagonal, 0.0).astype(BF16)
        block = factor_ref[start : start + base, start : start + base]
        inner_row = lax.broadcasted_iota(jnp.int32, block.shape, 0)
        inner_column = lax.broadcasted_iota(jnp.int32, block.shape, 1)
        on = jnp.sum(jnp.where(inner_row == inner_column, block, 0.0), axis=0, keepdims=True)
        dinv_ref[:, start : start + base] = 1.0 / on
        power = -n_ref[start : start + base, start : start + base].astype(F32)
        powers.append(power)
        totals.append(power)
    reach = 2
    while reach < base:
        for index in range(len(powers)):
            low = powers[index].astype(BF16)
            square = dot(low, low)
            low = square.astype(BF16)
            totals[index] = totals[index] + square + dot(totals[index].astype(BF16), low)
            powers[index] = square
        reach *= 2
    for index, start in enumerate(range(0, size, base)):
        t_ref[start : start + base, start : start + base] = totals[index].astype(BF16)
    width = base
    while width < size:
        for start in range(0, size, 2 * width):
            top = slice(start, start + width)
            bottom = slice(start + width, start + 2 * width)
            below = n_ref[bottom, top]
            first = below.astype(F32) + dot(below, t_ref[top, top])
            second = first + dot(t_ref[bottom, bottom], first.astype(BF16))
            t_ref[bottom, top] = (-second).astype(BF16)
        width *= 2


def lower(rows, t_ref):
    size = t_ref.shape[0]
    step = min(256, size)
    pieces = [dot_nt(rows[:, : i + step], t_ref[i : i + step, : i + step]) for i in range(0, size, step)]
    return jnp.concatenate(pieces, axis=1)


def lower_flipped(rows, t_ref):
    size = t_ref.shape[0]
    step = min(256, size)
    pieces = [dot(rows[:, i:], t_ref[i:, i : i + step]) for i in range(0, size, step)]
    return jnp.concatenate(pieces, axis=1)


def admm_kernel(
    sizes,
    offset,
    scale,
    penalty_hbm,
    samples_hbm,
    targets_hbm,
    member_hbm,
    omega_hbm,
    phase_hbm,
    factor_hbm,
    weights_hbm,
    duals_hbm,
    consensus_hbm,
    out_hbm,
    factor_ref,
    dinv_ref,
    strict_ref,
    solve_ref,
    samples_ref,
    targets_ref,
    member_ref,
    omega_ref,
    phase_ref,
    state_ref,
    penalty_ref,
    feat_ref,
    flip_ref,
    coarse_ref,
    acc_ref,
    part_ref,
    other_ref,
    resid_ref,
    gfar_ref,
    gside_ref,
    gown_ref,
    gsend_ref,
    grow_ref,
    rs_send_ref,
    rs_recv_ref,
    mean_ref,
    gap_ref,
    load_sem,
    store_sem,
    omega_send,
    omega_recv,
    phase_send,
    phase_recv,
    crow_send,
    crow_recv,
    cside_send,
    cside_recv,
    core_send,
    core_recv,
    gside_send,
    gside_recv,
    grow_send,
    grow_recv,
    rs_send,
    rs_recv,
    mean_send,
    mean_recv,
    gap_send,
    gap_recv,
):
    n_region, n_feat, n_row = sizes
    narrow, width = weights_hbm.shape
    outputs = n_row * narrow
    lanes = width // 128
    inputs = omega_hbm.shape[0]
    gain = scale * WAVE_GAIN
    count = feat_ref.shape[2]
    chunk = min(CHUNK, count)
    chunks = count // chunk
    piece_width = width // PARTS
    tile = min(512, piece_width)
    small = tile // 2
    ratio, tiles, pieces = tile // small, width // tile, width // small
    region, feat, row = lax.axis_index("region"), lax.axis_index("feat"), lax.axis_index("row")
    group = n_feat * n_row
    place = feat * n_row + row
    side = (region, lax.rem(feat + CORES, n_feat), row)
    core = (region, feat + 1 - 2 * lax.rem(feat, CORES), row)

    def row_peer(k):
        return (region, feat, lax.rem(row + k, n_row))

    def region_peer(k):
        return (lax.rem(region + k, n_region), feat, row)

    def far_peer(k):
        return (region, lax.rem(feat + CORES, n_feat), lax.rem(row + k, n_row))

    def group_peer(k):
        other = lax.rem(place + k, group)
        return (region, other // n_row, lax.rem(other, n_row))

    def remote(src, dst, send, recv, device):
        return pltpu.make_async_remote_copy(
            src_ref=src, dst_ref=dst, send_sem=send, recv_sem=recv,
            device_id=device, device_id_type=MESH,
        )

    first = pl.multiple_of((feat // CORES) * count, 128)
    span = pl.ds(first, count)
    loads = [
        pltpu.make_async_copy(samples_hbm.at[span], samples_ref.at[:, :inputs], load_sem.at[0]),
        pltpu.make_async_copy(omega_hbm, omega_ref.at[0], load_sem.at[1]),
        pltpu.make_async_copy(phase_hbm, phase_ref.at[0], load_sem.at[2]),
        pltpu.make_async_copy(weights_hbm, state_ref.at[0], load_sem.at[3]),
        pltpu.make_async_copy(duals_hbm, state_ref.at[1], load_sem.at[4]),
        pltpu.make_async_copy(consensus_hbm, state_ref.at[2], load_sem.at[5]),
        pltpu.make_async_copy(penalty_hbm, penalty_ref, load_sem.at[9]),
        pltpu.make_async_copy(targets_hbm.at[:, span], targets_ref, load_sem.at[6]),
        pltpu.make_async_copy(member_hbm.at[:, span], member_ref, load_sem.at[7]),
        pltpu.make_async_copy(factor_hbm, factor_ref, load_sem.at[8]),
    ]
    for load in loads[:7]:
        load.start()

    barrier = pltpu.get_barrier_semaphore()
    for k in range(1, group):
        pl.semaphore_signal(barrier, inc=1, device_id=group_peer(k), device_id_type=MESH)
    for k in range(1, n_region):
        pl.semaphore_signal(barrier, inc=1, device_id=region_peer(k), device_id_type=MESH)

    def column_of(line):
        pieces = []
        for j in range(line.shape[1] // 128):
            level = lax.broadcasted_iota(jnp.int32, (128, 128), 0)
            across = lax.broadcasted_iota(jnp.int32, (128, 128), 1)
            only = jnp.where(level == across, line[:, 128 * j : 128 * (j + 1)], 0.0)
            pieces.append(jnp.sum(only, axis=1, keepdims=True))
        return jnp.concatenate(pieces, axis=0)

    def omega_piece(i):
        span = pl.ds(pl.multiple_of(i * small, small), small)
        return remote(
            omega_ref.at[0, :, span], omega_ref.at[1, :, span], omega_send.at[i], omega_recv.at[i],
            side,
        )

    def phase_copy():
        return remote(phase_ref.at[0], phase_ref.at[1], phase_send.at[0], phase_recv.at[0], side)

    def near_copies(t):
        mine = coarse_ref.at[t, 0, row]
        return [
            remote(mine, mine, crow_send.at[t], crow_recv.at[t], row_peer(k))
            for k in range(1, n_row)
        ]

    def far_copies(t):
        mine, there = coarse_ref.at[t, 0, row], coarse_ref.at[t, 1, row]
        return [
            remote(mine, there, cside_send.at[t], cside_recv.at[t], far_peer(k))
            for k in range(n_row)
        ]

    def arrived(pieces, semaphore):
        remote(pieces, pieces, semaphore, semaphore, side).wait_recv()

    def sent(pieces, semaphore):
        remote(pieces, pieces, semaphore, semaphore, side).wait_send()

    def core_copy(t, j):
        return remote(
            part_ref.at[t, j], other_ref.at[t, j], core_send.at[t, j], core_recv.at[t, j], core
        )

    def start(copies):
        for copy in copies:
            copy.start()

    def fill(half, down, size):
        rows = pl.ds(pl.multiple_of(down, size), size)
        part = (omega_ref[half, :, rows].astype(F32) * INV_TURN).T
        high = part.astype(BF16)
        low = (part - high.astype(F32)).astype(BF16)
        column = column_of(phase_ref[half, :, rows] * INV_TURN)
        both = jnp.concatenate([high, low], axis=1)
        value = feature_tile(both, column, samples_ref[...])
        feat_ref[half, rows, :] = value
        flip_ref[half, :, rows] = value.T

    def fill_small(i, carry):
        omega_piece(i).wait_recv()
        fill(1, i * small, small)
        return carry

    def fill_large(i, carry):
        @pl.when(i == 1)
        def _():
            pl.semaphore_wait(barrier, group - 1 + n_region - 1)
            start([phase_copy()])
            start([omega_piece(j) for j in range(pieces)])
            coarse_ref[0, 0, row] = state_ref[0].astype(BF16)
            start(near_copies(0))
            start(far_copies(0))

        @pl.when(i == tiles)
        def _():
            phase_copy().wait_recv()
            lax.fori_loop(0, ratio, fill_small, 0)

        @pl.when(i >= tiles)
        def _():
            for j in range(ratio):
                omega_piece(ratio * lax.rem(i + 1, tiles) + j).wait_recv()

        half = i // tiles
        fill(half, (i - half * (tiles - 1)) * tile, tile)
        return carry

    history = jnp.zeros((1, 128), F32)
    lane = lax.broadcasted_iota(jnp.int32, (1, 128), 1)
    with jax.named_scope("load0"):
        for load in loads[:7]:
            load.wait()
        for load in loads[7:]:
            load.start()
        samples_ref[:, inputs:] = samples_ref[:, :inputs]
    with jax.named_scope("fill"):
        lax.fori_loop(0, 2 * tiles - 1, fill_large, 0)
    weights, duals, consensus = state_ref[0], state_ref[1], state_ref[2]
    rho = jnp.broadcast_to(penalty_ref[...], (1, 128))

    for t in range(ITERS):
        with jax.named_scope("near_wait"):
            arrived(coarse_ref.at[t, 0, pl.ds(0, n_row - 1)], crow_recv.at[t])
        if t == 0:
            loads[7].wait()
            loads[8].wait()
        with jax.named_scope("pred_near"):
            near = coarse_ref[t, 0].reshape(outputs, width)
            for j in range(chunks):
                span = slice(j * chunk, (j + 1) * chunk)
                acc_ref[:, span] = dot(near, feat_ref[0, :, span])
        with jax.named_scope("far_wait"):
            arrived(coarse_ref.at[t, 1], cside_recv.at[t])
        with jax.named_scope("pred_far"):
            far = coarse_ref[t, 1].reshape(outputs, width)
            for j in range(chunks):
                if t > 0 and j == chunks - 1:
                    with jax.named_scope("share_mean"):
                        share_mean(t - 1)
                span = slice(j * chunk, (j + 1) * chunk)
                part = gain * (acc_ref[:, span] + dot(far, feat_ref[1, :, span]))
                acc_ref[:, span] = part
                part_ref[t, j] = part.astype(BF16)
                core_copy(t, j).start()
        with jax.named_scope("resid"):
            for j in range(chunks):
                span = slice(j * chunk, (j + 1) * chunk)
                core_copy(t, j).wait_recv()
                predicted = acc_ref[:, span] + other_ref[t, j].astype(F32)
                gap_value = predicted - targets_ref[:, span].astype(F32)
                resid_ref[:, span] = (member_ref[:, span].astype(F32) * gap_value).astype(BF16)

        with jax.named_scope("grad_far"):
            for p in range(PARTS):
                span = slice(p * piece_width, (p + 1) * piece_width)
                value = dot(resid_ref[...], flip_ref[1, :, span])
                gfar_ref[t, p] = value.astype(BF16).reshape(n_row, narrow, piece_width)
                for k in range(n_row):
                    target = lax.rem(row + k, n_row)
                    copy = remote(
                        gfar_ref.at[t, p, target], gside_ref.at[t, p, k], gside_send.at[t],
                        gside_recv.at[t], far_peer(k),
                    )
                    copy.start()
        with jax.named_scope("grad_near"):
            for p in range(PARTS):
                span = slice(p * piece_width, (p + 1) * piece_width)
                value = dot(resid_ref[...], flip_ref[0, :, span])
                value = value.reshape(n_row, narrow, piece_width)
                gown_ref[p] = value
                gsend_ref[t, p] = value.astype(BF16)
                for k in range(1, n_row):
                    target = lax.rem(row + k, n_row)
                    copy = remote(
                        gsend_ref.at[t, p, target], grow_ref.at[t, p, k], grow_send.at[t],
                        grow_recv.at[t], row_peer(k),
                    )
                    copy.start()
        if t == 0:
            with jax.named_scope("invert"):
                loads[9].wait()
                invert(min(256, width), factor_ref, dinv_ref, strict_ref, solve_ref)
        else:
            with jax.named_scope("finish_region"):
                apart, duals, consensus = finish_region(t - 1)
        dinv = dinv_ref[...]
        with jax.named_scope("grad_wait"):
            arrived(gside_ref.at[t], gside_recv.at[t])
            arrived(grow_ref.at[t, :, pl.ds(1, n_row - 1)], grow_recv.at[t])
            gradient = []
            for p in range(PARTS):
                value = gown_ref[p, row]
                for k in range(n_row):
                    value = value + gside_ref[t, p, k].astype(F32)
                for k in range(1, n_row):
                    value = value + grow_ref[t, p, k].astype(F32)
                gradient.append(value)
            gradient = gain * jnp.concatenate(gradient, axis=1)
        with jax.named_scope("solve"):
            scalar = rho[:, :1]
            if t == 0:
                right = gradient + scalar * (weights - consensus + duals)
            else:
                right = jnp.concatenate([gradient + scalar * duals, apart], axis=0)
            forward = right * dinv
            forward = forward + lower(forward.astype(BF16), solve_ref)
            update = (forward + lower_flipped(forward.astype(BF16), solve_ref)) * dinv
        if t > 0:
            with jax.named_scope("finish_gap"):
                rho, duals, history = finish_gap(t - 1, rho, duals, history)
            scalar = rho[:, :1]
            update = update[:narrow] + scalar * update[narrow:]
        weights = weights - update
        if t < ITERS - 1:
            coarse_ref[t + 1, 0, row] = weights.astype(BF16)
            start(near_copies(t + 1))

        total = scalar * (weights + duals)
        for c in range(n_region):
            down, right = 8 * (c // lanes), 128 * (c % lanes)
            rs_send_ref[t, c, :8] = total[down : down + 8, right : right + 128]
            rs_send_ref[t, c, 8:] = jnp.broadcast_to(scalar, (8, 128))
        rs_recv_ref[t, region] = rs_send_ref[t, region]
        for k in range(1, n_region):
            owner = lax.rem(region + k, n_region)
            copy = remote(
                rs_send_ref.at[t, owner, pl.ds(0, 9)], rs_recv_ref.at[t, region, pl.ds(0, 9)],
                rs_send.at[t], rs_recv.at[t], region_peer(k),
            )
            copy.start()
        if t < ITERS - 1:
            start(far_copies(t + 1))

        def share_mean(s):
            arrived(rs_recv_ref.at[s, pl.ds(0, n_region - 1), pl.ds(0, 9)], rs_recv.at[s])
            total = rs_recv_ref[s, 0, :9]
            for r in range(1, n_region):
                total = total + rs_recv_ref[s, r, :9]
            mean_ref[s, region] = total[:8] / total[8:9]
            mine = mean_ref.at[s, region]
            for k in range(1, n_region):
                remote(mine, mine, mean_send.at[s], mean_recv.at[s], region_peer(k)).start()

        def finish_region(s, weights=weights, duals=duals, consensus=consensus):
            arrived(mean_ref.at[s, pl.ds(0, n_region - 1)], mean_recv.at[s])
            updated = jnp.concatenate(
                [
                    jnp.concatenate([mean_ref[s, h * lanes + j] for j in range(lanes)], axis=1)
                    for h in range(narrow // 8)
                ],
                axis=0,
            )
            gap = jnp.sum(jnp.square(weights - updated), keepdims=True).reshape(1, 1)
            drift = jnp.sum(jnp.square(updated - consensus), keepdims=True).reshape(1, 1)
            gap_ref[s, place, :1] = jnp.where(lane < 64, gap, drift)
            mine = gap_ref.at[s, place, pl.ds(0, 1)]
            for k in range(1, group):
                remote(mine, mine, gap_send.at[s], gap_recv.at[s], group_peer(k)).start()
            return weights - updated, duals + weights - updated, updated

        def finish_gap(s, rho, duals, history):
            arrived(gap_ref.at[s, pl.ds(0, group - 1), pl.ds(0, 1)], gap_recv.at[s])
            total = jnp.sum(gap_ref[s, :, :1], axis=0)
            gap = jnp.broadcast_to(total[:, :1], (1, 128))
            drift = jnp.broadcast_to(total[:, 64:65], (1, 128))
            drift = rho * rho * drift
            renewed = rho * jnp.sqrt((gap + offset) / (drift + offset))
            duals = duals * (rho / renewed)[:, :1]
            return renewed, duals, jnp.where(lane == s, renewed, history)

    def store(rows, value):
        state_ref[rows] = value
        copy = pltpu.make_async_copy(state_ref.at[rows], out_hbm.at[rows], store_sem.at[rows])
        copy.start()
        return copy

    stores = [store(0, weights)]
    with jax.named_scope("drain_early"):
        phase_copy().wait_send()
        for i in range(pieces):
            omega_piece(i).wait_send()
        for t in range(ITERS):
            sent(coarse_ref.at[t, 0, pl.ds(0, n_row - 1)], crow_send.at[t])
            sent(coarse_ref.at[t, 1], cside_send.at[t])
            for j in range(chunks):
                core_copy(t, j).wait_send()
            sent(gside_ref.at[t], gside_send.at[t])
            sent(grow_ref.at[t, :, pl.ds(1, n_row - 1)], grow_send.at[t])
            sent(rs_recv_ref.at[t, pl.ds(0, n_region - 1), pl.ds(0, 9)], rs_send.at[t])
            if t < ITERS - 1:
                sent(mean_ref.at[t, pl.ds(0, n_region - 1)], mean_send.at[t])
                sent(gap_ref.at[t, pl.ds(0, group - 1), pl.ds(0, 1)], gap_send.at[t])
    with jax.named_scope("last_mean"):
        share_mean(ITERS - 1)
    with jax.named_scope("last_region"):
        apart, duals, consensus = finish_region(ITERS - 1)
    stores.append(store(2, consensus))
    with jax.named_scope("last_gap"):
        rho, duals, history = finish_gap(ITERS - 1, rho, duals, history)
    stores.append(store(1, duals))
    stores.append(store(3, jnp.broadcast_to(jnp.tile(history, (1, width // 128)), (narrow, width))))
    with jax.named_scope("drain"):
        sent(mean_ref.at[ITERS - 1, pl.ds(0, n_region - 1)], mean_send.at[ITERS - 1])
        sent(gap_ref.at[ITERS - 1, pl.ds(0, group - 1), pl.ds(0, 1)], gap_send.at[ITERS - 1])
        for copy in stores:
            copy.wait()


def admm(sizes, offset, scale, penalty, samples, targets, member, omega, phase, factors, *state):
    n_region, n_feat, n_row = sizes
    narrow, width = state[0].shape
    outputs = n_row * narrow
    inputs = omega.shape[0]
    count = samples.shape[0] // (n_feat // CORES)
    chunk = min(CHUNK, count)
    chunks = count // chunk
    group = n_feat * n_row
    part = (n_row, narrow, width // PARTS)
    tiles = width // min(512, width // PARTS)
    hbm = pl.BlockSpec(memory_space=pl.ANY)
    dma = pltpu.SemaphoreType.DMA
    return pl.pallas_call(
        functools.partial(admm_kernel, sizes, offset, scale),
        in_specs=[hbm] * 10,
        out_specs=hbm,
        out_shape=jax.ShapeDtypeStruct((4, narrow, width), F32),
        scratch_shapes=[
            pltpu.VMEM((width, width), F32),
            pltpu.VMEM((1, width), F32),
            pltpu.VMEM((width, width), BF16),
            pltpu.VMEM((width, width), BF16),
            pltpu.VMEM((count, 2 * inputs), BF16),
            pltpu.VMEM((outputs, count), BF16),
            pltpu.VMEM((1, count), jnp.int32),
            pltpu.VMEM((2, inputs, width), BF16),
            pltpu.VMEM((2, 1, width), F32),
            pltpu.VMEM((4, narrow, width), F32),
            pltpu.VMEM((1, 1), F32),
            pltpu.VMEM((2, width, count), BF16),
            pltpu.VMEM((2, count, width), BF16),
            pltpu.VMEM((ITERS, 2, n_row, narrow, width), BF16),
            pltpu.VMEM((outputs, count), F32),
            pltpu.VMEM((ITERS, chunks, outputs, chunk), BF16),
            pltpu.VMEM((ITERS, chunks, outputs, chunk), BF16),
            pltpu.VMEM((outputs, count), BF16),
            pltpu.VMEM((ITERS, PARTS) + part, BF16),
            pltpu.VMEM((ITERS, PARTS) + part, BF16),
            pltpu.VMEM((PARTS,) + part, F32),
            pltpu.VMEM((ITERS, PARTS) + part, BF16),
            pltpu.VMEM((ITERS, PARTS) + part, BF16),
            pltpu.VMEM((ITERS, n_region, 16, 128), F32),
            pltpu.VMEM((ITERS, n_region, 16, 128), F32),
            pltpu.VMEM((ITERS, n_region, 8, 128), F32),
            pltpu.VMEM((ITERS, group, 8, 128), F32),
            dma((10,)),
            dma((4,)),
            dma((2 * tiles,)),
            dma((2 * tiles,)),
            dma((1,)),
            dma((1,)),
            dma((ITERS,)),
            dma((ITERS,)),
            dma((ITERS,)),
            dma((ITERS,)),
            dma((ITERS, chunks)),
            dma((ITERS, chunks)),
            dma((ITERS,)),
            dma((ITERS,)),
            dma((ITERS,)),
            dma((ITERS,)),
            dma((ITERS,)),
            dma((ITERS,)),
            dma((ITERS,)),
            dma((ITERS,)),
            dma((ITERS,)),
            dma((ITERS,)),
        ],
        compiler_params=pltpu.CompilerParams(
            collective_id=0, has_side_effects=True, vmem_limit_bytes=63 * 2**20
        ),
        name="admm",
    )(penalty, samples, targets, member, omega, phase, factors, *state)


def per_device(
    sizes,
    samples,
    targets,
    member,
    omega,
    phase,
    factors,
    weights_init,
    duals_init,
    consensus_init,
    penalty_init,
):
    n_region, n_feat, n_row = sizes
    total_features = n_feat * omega.shape[1]
    total_outputs = targets.shape[1]
    offset = 0.01 * total_features * total_outputs
    scale = math.sqrt(2.0 / total_features)
    final = admm(
        sizes, offset, scale, penalty_init[None, :], samples, targets.T, member[None, :], omega,
        phase[None, :], factors, weights_init.T, duals_init.T, consensus_init.T,
    )
    return (final[0].T, final[1].T, final[2].T, final[3, :1, :ITERS])


def solution(mesh):
    sizes = (mesh.shape["region"], mesh.shape["feat"], mesh.shape["row"])
    return jax.shard_map(
        functools.partial(per_device, sizes),
        mesh=mesh,
        in_specs=(
            P(("region", "row"), None),
            P(("region", "row"), None),
            P(("region", "row")),
            P(None, "feat"),
            P("feat"),
            P(("region", "feat"), None),
            P(("region", "feat"), "row"),
            P(("region", "feat"), "row"),
            P("feat", "row"),
            P("region"),
        ),
        out_specs=(
            P(("region", "feat"), "row"),
            P(("region", "feat"), "row"),
            P("feat", "row"),
            P("region", None),
        ),
        check_vma=False,
    )
```

```python
import functools
import math

import jax
import jax.numpy as jnp
from jax import lax
from jax.experimental import pallas as pl
from jax.experimental.pallas import tpu as pltpu
from jax.sharding import PartitionSpec as P

ITERS = 3
CORES = 2
PARTS = 2
CHUNK = 2048
MESH = pl.DeviceIdType.MESH
INV_TURN = 1.0 / (2.0 * math.pi)
WAVE_GAIN, WAVE_MIDDLE, WAVE_LAST = 71.848585, -0.5703125, 0.08740234375
F32 = jnp.float32
BF16 = jnp.bfloat16


def dot(a, b):
    return lax.dot_general(a, b, (((1,), (0,)), ((), ())), preferred_element_type=F32)


def dot_nt(a, b):
    return lax.dot_general(a, b, (((1,), (1,)), ((), ())), preferred_element_type=F32)


def feature_tile(omega, phase, samples):
    turns = dot_nt(omega, samples) + phase
    rest = (0.25 - jnp.abs(turns - jnp.round(turns))).astype(BF16)
    square = rest * rest
    value = (square + jnp.asarray(WAVE_MIDDLE, BF16)) * square + jnp.asarray(WAVE_LAST, BF16)
    return value * rest


def invert(base, factor_ref, dinv_ref, n_ref, t_ref):
    size = factor_ref.shape[0]
    t_ref[...] = jnp.zeros_like(t_ref)
    powers, totals = [], []
    for start in range(0, size, base):
        rows = factor_ref[start : start + base, :]
        row = lax.broadcasted_iota(jnp.int32, rows.shape, 0) + start
        column = lax.broadcasted_iota(jnp.int32, rows.shape, 1)
        diagonal = jnp.sum(jnp.where(row == column, rows, 0.0), axis=1, keepdims=True)
        n_ref[start : start + base, :] = jnp.where(row > column, rows / diagonal, 0.0).astype(BF16)
        block = factor_ref[start : start + base, start : start + base]
        inner_row = lax.broadcasted_iota(jnp.int32, block.shape, 0)
        inner_column = lax.broadcasted_iota(jnp.int32, block.shape, 1)
        on = jnp.sum(jnp.where(inner_row == inner_column, block, 0.0), axis=0, keepdims=True)
        dinv_ref[:, start : start + base] = 1.0 / on
        power = -n_ref[start : start + base, start : start + base].astype(F32)
        powers.append(power)
        totals.append(power)
    reach = 2
    while reach < base:
        for index in range(len(powers)):
            low = powers[index].astype(BF16)
            square = dot(low, low)
            low = square.astype(BF16)
            totals[index] = totals[index] + square + dot(totals[index].astype(BF16), low)
            powers[index] = square
        reach *= 2
    for index, start in enumerate(range(0, size, base)):
        t_ref[start : start + base, start : start + base] = totals[index].astype(BF16)
    width = base
    while width < size:
        for start in range(0, size, 2 * width):
            top = slice(start, start + width)
            bottom = slice(start + width, start + 2 * width)
            below = n_ref[bottom, top]
            first = below.astype(F32) + dot(below, t_ref[top, top])
            second = first + dot(t_ref[bottom, bottom], first.astype(BF16))
            t_ref[bottom, top] = (-second).astype(BF16)
        width *= 2


def lower(rows, t_ref):
    size = t_ref.shape[0]
    step = min(256, size)
    pieces = [dot_nt(rows[:, : i + step], t_ref[i : i + step, : i + step]) for i in range(0, size, step)]
    return jnp.concatenate(pieces, axis=1)


def lower_flipped(rows, t_ref):
    size = t_ref.shape[0]
    step = min(256, size)
    pieces = [dot(rows[:, i:], t_ref[i:, i : i + step]) for i in range(0, size, step)]
    return jnp.concatenate(pieces, axis=1)


def admm_kernel(
    sizes,
    offset,
    scale,
    penalty_hbm,
    samples_hbm,
    targets_hbm,
    member_hbm,
    omega_hbm,
    phase_hbm,
    factor_hbm,
    weights_hbm,
    duals_hbm,
    consensus_hbm,
    out_hbm,
    factor_ref,
    dinv_ref,
    strict_ref,
    solve_ref,
    samples_ref,
    targets_ref,
    member_ref,
    omega_ref,
    phase_ref,
    state_ref,
    penalty_ref,
    feat_ref,
    flip_ref,
    coarse_ref,
    acc_ref,
    part_ref,
    other_ref,
    resid_ref,
    gfar_ref,
    gside_ref,
    gown_ref,
    gsend_ref,
    grow_ref,
    rs_send_ref,
    rs_recv_ref,
    mean_ref,
    gap_ref,
    load_sem,
    store_sem,
    omega_send,
    omega_recv,
    phase_send,
    phase_recv,
    crow_send,
    crow_recv,
    cside_send,
    cside_recv,
    core_send,
    core_recv,
    gside_send,
    gside_recv,
    grow_send,
    grow_recv,
    rs_send,
    rs_recv,
    mean_send,
    mean_recv,
    gap_send,
    gap_recv,
):
    n_region, n_feat, n_row = sizes
    narrow, width = weights_hbm.shape
    outputs = n_row * narrow
    lanes = width // 128
    inputs = omega_hbm.shape[0]
    gain = scale * WAVE_GAIN
    count = feat_ref.shape[2]
    chunk = min(CHUNK, count)
    chunks = count // chunk
    piece_width = width // PARTS
    tile = min(512, piece_width)
    small = tile // 2
    ratio, tiles, pieces = tile // small, width // tile, width // small
    region, feat, row = lax.axis_index("region"), lax.axis_index("feat"), lax.axis_index("row")
    group = n_feat * n_row
    place = feat * n_row + row
    side = (region, lax.rem(feat + CORES, n_feat), row)
    core = (region, feat + 1 - 2 * lax.rem(feat, CORES), row)

    def apart_rows(k):
        return min(k % n_row, n_row - k % n_row)

    def apart_regions(k):
        return min(k // CORES, n_region // CORES - k // CORES) + 2 * (k % CORES)

    def apart_group(k):
        return apart_rows(k) + 0.5 * min(k // n_row, n_feat - k // n_row)

    near_order = sorted(range(1, n_row), key=apart_rows, reverse=True)
    far_order = sorted(range(n_row), key=apart_rows, reverse=True)
    region_order = sorted(range(1, n_region), key=apart_regions, reverse=True)
    group_order = sorted(range(1, group), key=apart_group, reverse=True)

    def row_peer(k):
        return (region, feat, lax.rem(row + k, n_row))

    def region_peer(k):
        return (lax.rem(region + k, n_region), feat, row)

    def far_peer(k):
        return (region, lax.rem(feat + CORES, n_feat), lax.rem(row + k, n_row))

    def group_peer(k):
        other = lax.rem(place + k, group)
        return (region, other // n_row, lax.rem(other, n_row))

    def remote(src, dst, send, recv, device):
        return pltpu.make_async_remote_copy(
            src_ref=src, dst_ref=dst, send_sem=send, recv_sem=recv,
            device_id=device, device_id_type=MESH,
        )

    first = pl.multiple_of((feat // CORES) * count, 128)
    span = pl.ds(first, count)
    loads = [
        pltpu.make_async_copy(samples_hbm.at[span], samples_ref.at[:, :inputs], load_sem.at[0]),
        pltpu.make_async_copy(omega_hbm, omega_ref.at[0], load_sem.at[1]),
        pltpu.make_async_copy(phase_hbm, phase_ref.at[0], load_sem.at[2]),
        pltpu.make_async_copy(weights_hbm, state_ref.at[0], load_sem.at[3]),
        pltpu.make_async_copy(duals_hbm, state_ref.at[1], load_sem.at[4]),
        pltpu.make_async_copy(consensus_hbm, state_ref.at[2], load_sem.at[5]),
        pltpu.make_async_copy(penalty_hbm, penalty_ref, load_sem.at[9]),
        pltpu.make_async_copy(targets_hbm.at[:, span], targets_ref, load_sem.at[6]),
        pltpu.make_async_copy(member_hbm.at[:, span], member_ref, load_sem.at[7]),
        pltpu.make_async_copy(factor_hbm, factor_ref, load_sem.at[8]),
    ]
    for load in loads[:7]:
        load.start()

    barrier = pltpu.get_barrier_semaphore()
    for k in group_order:
        pl.semaphore_signal(barrier, inc=1, device_id=group_peer(k), device_id_type=MESH)
    for k in region_order:
        pl.semaphore_signal(barrier, inc=1, device_id=region_peer(k), device_id_type=MESH)

    def column_of(line):
        pieces = []
        for j in range(line.shape[1] // 128):
            level = lax.broadcasted_iota(jnp.int32, (128, 128), 0)
            across = lax.broadcasted_iota(jnp.int32, (128, 128), 1)
            only = jnp.where(level == across, line[:, 128 * j : 128 * (j + 1)], 0.0)
            pieces.append(jnp.sum(only, axis=1, keepdims=True))
        return jnp.concatenate(pieces, axis=0)

    def omega_piece(i):
        span = pl.ds(pl.multiple_of(i * small, small), small)
        return remote(
            omega_ref.at[0, :, span], omega_ref.at[1, :, span], omega_send.at[i], omega_recv.at[i],
            side,
        )

    def phase_copy():
        return remote(phase_ref.at[0], phase_ref.at[1], phase_send.at[0], phase_recv.at[0], side)

    def near_copies(t):
        mine = coarse_ref.at[t, 0, row]
        return [
            remote(mine, mine, crow_send.at[t], crow_recv.at[t], row_peer(k))
            for k in near_order
        ]

    def far_copies(t):
        mine, there = coarse_ref.at[t, 0, row], coarse_ref.at[t, 1, row]
        return [
            remote(mine, there, cside_send.at[t], cside_recv.at[t], far_peer(k))
            for k in far_order
        ]

    def arrived(pieces, semaphore):
        remote(pieces, pieces, semaphore, semaphore, side).wait_recv()

    def sent(pieces, semaphore):
        remote(pieces, pieces, semaphore, semaphore, side).wait_send()

    def core_copy(t, j):
        return remote(
            part_ref.at[t, j], other_ref.at[t, j], core_send.at[t, j], core_recv.at[t, j], core
        )

    def start(copies):
        for copy in copies:
            copy.start()

    def fill(half, down, size):
        rows = pl.ds(pl.multiple_of(down, size), size)
        part = (omega_ref[half, :, rows].astype(F32) * INV_TURN).T
        high = part.astype(BF16)
        low = (part - high.astype(F32)).astype(BF16)
        column = column_of(phase_ref[half, :, rows] * INV_TURN)
        both = jnp.concatenate([high, low], axis=1)
        value = feature_tile(both, column, samples_ref[...])
        feat_ref[half, rows, :] = value
        flip_ref[half, :, rows] = value.T

    def fill_small(i, carry):
        omega_piece(i).wait_recv()
        fill(1, i * small, small)
        return carry

    def fill_large(i, carry):
        @pl.when(i == 1)
        def _():
            pl.semaphore_wait(barrier, group - 1 + n_region - 1)
            start([phase_copy()])
            start([omega_piece(j) for j in range(pieces)])
            coarse_ref[0, 0, row] = state_ref[0].astype(BF16)
            start(near_copies(0))
            start(far_copies(0))

        @pl.when(i == tiles)
        def _():
            phase_copy().wait_recv()
            lax.fori_loop(0, ratio, fill_small, 0)

        @pl.when(i >= tiles)
        def _():
            for j in range(ratio):
                omega_piece(ratio * lax.rem(i + 1, tiles) + j).wait_recv()

        half = i // tiles
        fill(half, (i - half * (tiles - 1)) * tile, tile)
        return carry

    history = jnp.zeros((1, 128), F32)
    lane = lax.broadcasted_iota(jnp.int32, (1, 128), 1)
    with jax.named_scope("load0"):
        for load in loads[:7]:
            load.wait()
        for load in loads[7:]:
            load.start()
        samples_ref[:, inputs:] = samples_ref[:, :inputs]
    with jax.named_scope("fill"):
        lax.fori_loop(0, 2 * tiles - 1, fill_large, 0)
    weights, duals, consensus = state_ref[0], state_ref[1], state_ref[2]
    rho = jnp.broadcast_to(penalty_ref[...], (1, 128))

    for t in range(ITERS):
        with jax.named_scope("near_wait"):
            arrived(coarse_ref.at[t, 0, pl.ds(0, n_row - 1)], crow_recv.at[t])
        if t == 0:
            loads[7].wait()
            loads[8].wait()
        with jax.named_scope("pred_near"):
            near = coarse_ref[t, 0].reshape(outputs, width)
            for j in range(chunks):
                span = slice(j * chunk, (j + 1) * chunk)
                acc_ref[:, span] = dot(near, feat_ref[0, :, span])
        if t > 0:
            with jax.named_scope("share_mean"):
                share_mean(t - 1)
        with jax.named_scope("far_wait"):
            arrived(coarse_ref.at[t, 1], cside_recv.at[t])
        with jax.named_scope("pred_far"):
            far = coarse_ref[t, 1].reshape(outputs, width)
            for j in range(chunks):
                span = slice(j * chunk, (j + 1) * chunk)
                part = gain * (acc_ref[:, span] + dot(far, feat_ref[1, :, span]))
                acc_ref[:, span] = part
                part_ref[t, j] = part.astype(BF16)
                core_copy(t, j).start()
        with jax.named_scope("resid"):
            for j in range(chunks):
                span = slice(j * chunk, (j + 1) * chunk)
                core_copy(t, j).wait_recv()
                predicted = acc_ref[:, span] + other_ref[t, j].astype(F32)
                gap_value = predicted - targets_ref[:, span].astype(F32)
                resid_ref[:, span] = (member_ref[:, span].astype(F32) * gap_value).astype(BF16)

        with jax.named_scope("grad_far"):
            for p in range(PARTS):
                span = slice(p * piece_width, (p + 1) * piece_width)
                value = dot(resid_ref[...], flip_ref[1, :, span])
                gfar_ref[t, p] = value.astype(BF16).reshape(n_row, narrow, piece_width)
                for k in far_order:
                    target = lax.rem(row + k, n_row)
                    copy = remote(
                        gfar_ref.at[t, p, target], gside_ref.at[t, p, k], gside_send.at[t],
                        gside_recv.at[t], far_peer(k),
                    )
                    copy.start()
        with jax.named_scope("grad_near"):
            for p in range(PARTS):
                span = slice(p * piece_width, (p + 1) * piece_width)
                value = dot(resid_ref[...], flip_ref[0, :, span])
                value = value.reshape(n_row, narrow, piece_width)
                gown_ref[p] = value
                gsend_ref[t, p] = value.astype(BF16)
                for k in near_order:
                    target = lax.rem(row + k, n_row)
                    copy = remote(
                        gsend_ref.at[t, p, target], grow_ref.at[t, p, k], grow_send.at[t],
                        grow_recv.at[t], row_peer(k),
                    )
                    copy.start()
        if t == 0:
            with jax.named_scope("invert"):
                loads[9].wait()
                invert(min(256, width), factor_ref, dinv_ref, strict_ref, solve_ref)
        else:
            with jax.named_scope("finish_region"):
                apart, duals, consensus = finish_region(t - 1)
        dinv = dinv_ref[...]
        with jax.named_scope("grad_wait"):
            arrived(gside_ref.at[t], gside_recv.at[t])
            arrived(grow_ref.at[t, :, pl.ds(1, n_row - 1)], grow_recv.at[t])
            gradient = []
            for p in range(PARTS):
                value = gown_ref[p, row]
                for k in range(n_row):
                    value = value + gside_ref[t, p, k].astype(F32)
                for k in range(1, n_row):
                    value = value + grow_ref[t, p, k].astype(F32)
                gradient.append(value)
            gradient = gain * jnp.concatenate(gradient, axis=1)
        with jax.named_scope("solve"):
            scalar = rho[:, :1]
            if t == 0:
                right = gradient + scalar * (weights - consensus + duals)
            else:
                right = jnp.concatenate([gradient + scalar * duals, apart], axis=0)
            forward = right * dinv
            forward = forward + lower(forward.astype(BF16), solve_ref)
            update = (forward + lower_flipped(forward.astype(BF16), solve_ref)) * dinv
        if t > 0:
            with jax.named_scope("finish_gap"):
                rho, duals, history = finish_gap(t - 1, rho, duals, history)
            scalar = rho[:, :1]
            update = update[:narrow] + scalar * update[narrow:]
        weights = weights - update
        if t < ITERS - 1:
            coarse_ref[t + 1, 0, row] = weights.astype(BF16)
            start(near_copies(t + 1))

        total = scalar * (weights + duals)
        for c in range(n_region):
            down, right = 8 * (c // lanes), 128 * (c % lanes)
            rs_send_ref[t, c, :8] = total[down : down + 8, right : right + 128]
            rs_send_ref[t, c, 8:] = jnp.broadcast_to(scalar, (8, 128))
        rs_recv_ref[t, region] = rs_send_ref[t, region]
        for k in region_order:
            owner = lax.rem(region + k, n_region)
            copy = remote(
                rs_send_ref.at[t, owner, pl.ds(0, 9)], rs_recv_ref.at[t, region, pl.ds(0, 9)],
                rs_send.at[t], rs_recv.at[t], region_peer(k),
            )
            copy.start()
        if t < ITERS - 1:
            start(far_copies(t + 1))

        def share_mean(s):
            arrived(rs_recv_ref.at[s, pl.ds(0, n_region - 1), pl.ds(0, 9)], rs_recv.at[s])
            total = rs_recv_ref[s, 0, :9]
            for r in range(1, n_region):
                total = total + rs_recv_ref[s, r, :9]
            mean_ref[s, region] = total[:8] / total[8:9]
            mine = mean_ref.at[s, region]
            for k in region_order:
                remote(mine, mine, mean_send.at[s], mean_recv.at[s], region_peer(k)).start()

        def finish_region(s, weights=weights, duals=duals, consensus=consensus):
            arrived(mean_ref.at[s, pl.ds(0, n_region - 1)], mean_recv.at[s])
            updated = jnp.concatenate(
                [
                    jnp.concatenate([mean_ref[s, h * lanes + j] for j in range(lanes)], axis=1)
                    for h in range(narrow // 8)
                ],
                axis=0,
            )
            gap = jnp.sum(jnp.square(weights - updated), keepdims=True).reshape(1, 1)
            drift = jnp.sum(jnp.square(updated - consensus), keepdims=True).reshape(1, 1)
            gap_ref[s, place, :1] = jnp.where(lane < 64, gap, drift)
            mine = gap_ref.at[s, place, pl.ds(0, 1)]
            for k in group_order:
                remote(mine, mine, gap_send.at[s], gap_recv.at[s], group_peer(k)).start()
            return weights - updated, duals + weights - updated, updated

        def finish_gap(s, rho, duals, history):
            arrived(gap_ref.at[s, pl.ds(0, group - 1), pl.ds(0, 1)], gap_recv.at[s])
            total = jnp.sum(gap_ref[s, :, :1], axis=0)
            gap = jnp.broadcast_to(total[:, :1], (1, 128))
            drift = jnp.broadcast_to(total[:, 64:65], (1, 128))
            drift = rho * rho * drift
            renewed = rho * jnp.sqrt((gap + offset) / (drift + offset))
            duals = duals * (rho / renewed)[:, :1]
            return renewed, duals, jnp.where(lane == s, renewed, history)

    def store(rows, value):
        state_ref[rows] = value
        copy = pltpu.make_async_copy(state_ref.at[rows], out_hbm.at[rows], store_sem.at[rows])
        copy.start()
        return copy

    stores = [store(0, weights)]
    with jax.named_scope("drain_early"):
        phase_copy().wait_send()
        for i in range(pieces):
            omega_piece(i).wait_send()
        for t in range(ITERS):
            sent(coarse_ref.at[t, 0, pl.ds(0, n_row - 1)], crow_send.at[t])
            sent(coarse_ref.at[t, 1], cside_send.at[t])
            for j in range(chunks):
                core_copy(t, j).wait_send()
            sent(gside_ref.at[t], gside_send.at[t])
            sent(grow_ref.at[t, :, pl.ds(1, n_row - 1)], grow_send.at[t])
            sent(rs_recv_ref.at[t, pl.ds(0, n_region - 1), pl.ds(0, 9)], rs_send.at[t])
            if t < ITERS - 1:
                sent(mean_ref.at[t, pl.ds(0, n_region - 1)], mean_send.at[t])
                sent(gap_ref.at[t, pl.ds(0, group - 1), pl.ds(0, 1)], gap_send.at[t])
    with jax.named_scope("last_mean"):
        share_mean(ITERS - 1)
    with jax.named_scope("last_region"):
        apart, duals, consensus = finish_region(ITERS - 1)
    stores.append(store(2, consensus))
    with jax.named_scope("last_gap"):
        rho, duals, history = finish_gap(ITERS - 1, rho, duals, history)
    stores.append(store(1, duals))
    stores.append(store(3, jnp.broadcast_to(jnp.tile(history, (1, width // 128)), (narrow, width))))
    with jax.named_scope("drain"):
        sent(mean_ref.at[ITERS - 1, pl.ds(0, n_region - 1)], mean_send.at[ITERS - 1])
        sent(gap_ref.at[ITERS - 1, pl.ds(0, group - 1), pl.ds(0, 1)], gap_send.at[ITERS - 1])
        for copy in stores:
            copy.wait()


def admm(sizes, offset, scale, penalty, samples, targets, member, omega, phase, factors, *state):
    n_region, n_feat, n_row = sizes
    narrow, width = state[0].shape
    outputs = n_row * narrow
    inputs = omega.shape[0]
    count = samples.shape[0] // (n_feat // CORES)
    chunk = min(CHUNK, count)
    chunks = count // chunk
    group = n_feat * n_row
    part = (n_row, narrow, width // PARTS)
    tiles = width // min(512, width // PARTS)
    hbm = pl.BlockSpec(memory_space=pl.ANY)
    dma = pltpu.SemaphoreType.DMA
    return pl.pallas_call(
        functools.partial(admm_kernel, sizes, offset, scale),
        in_specs=[hbm] * 10,
        out_specs=hbm,
        out_shape=jax.ShapeDtypeStruct((4, narrow, width), F32),
        scratch_shapes=[
            pltpu.VMEM((width, width), F32),
            pltpu.VMEM((1, width), F32),
            pltpu.VMEM((width, width), BF16),
            pltpu.VMEM((width, width), BF16),
            pltpu.VMEM((count, 2 * inputs), BF16),
            pltpu.VMEM((outputs, count), BF16),
            pltpu.VMEM((1, count), jnp.int32),
            pltpu.VMEM((2, inputs, width), BF16),
            pltpu.VMEM((2, 1, width), F32),
            pltpu.VMEM((4, narrow, width), F32),
            pltpu.VMEM((1, 1), F32),
            pltpu.VMEM((2, width, count), BF16),
            pltpu.VMEM((2, count, width), BF16),
            pltpu.VMEM((ITERS, 2, n_row, narrow, width), BF16),
            pltpu.VMEM((outputs, count), F32),
            pltpu.VMEM((ITERS, chunks, outputs, chunk), BF16),
            pltpu.VMEM((ITERS, chunks, outputs, chunk), BF16),
            pltpu.VMEM((outputs, count), BF16),
            pltpu.VMEM((ITERS, PARTS) + part, BF16),
            pltpu.VMEM((ITERS, PARTS) + part, BF16),
            pltpu.VMEM((PARTS,) + part, F32),
            pltpu.VMEM((ITERS, PARTS) + part, BF16),
            pltpu.VMEM((ITERS, PARTS) + part, BF16),
            pltpu.VMEM((ITERS, n_region, 16, 128), F32),
            pltpu.VMEM((ITERS, n_region, 16, 128), F32),
            pltpu.VMEM((ITERS, n_region, 8, 128), F32),
            pltpu.VMEM((ITERS, group, 8, 128), F32),
            dma((10,)),
            dma((4,)),
            dma((2 * tiles,)),
            dma((2 * tiles,)),
            dma((1,)),
            dma((1,)),
            dma((ITERS,)),
            dma((ITERS,)),
            dma((ITERS,)),
            dma((ITERS,)),
            dma((ITERS, chunks)),
            dma((ITERS, chunks)),
            dma((ITERS,)),
            dma((ITERS,)),
            dma((ITERS,)),
            dma((ITERS,)),
            dma((ITERS,)),
            dma((ITERS,)),
            dma((ITERS,)),
            dma((ITERS,)),
            dma((ITERS,)),
            dma((ITERS,)),
        ],
        compiler_params=pltpu.CompilerParams(
            collective_id=0, has_side_effects=True, vmem_limit_bytes=63 * 2**20
        ),
        name="admm",
    )(penalty, samples, targets, member, omega, phase, factors, *state)


def per_device(
    sizes,
    samples,
    targets,
    member,
    omega,
    phase,
    factors,
    weights_init,
    duals_init,
    consensus_init,
    penalty_init,
):
    n_region, n_feat, n_row = sizes
    total_features = n_feat * omega.shape[1]
    total_outputs = targets.shape[1]
    offset = 0.01 * total_features * total_outputs
    scale = math.sqrt(2.0 / total_features)
    final = admm(
        sizes, offset, scale, penalty_init[None, :], samples, targets.T, member[None, :], omega,
        phase[None, :], factors, weights_init.T, duals_init.T, consensus_init.T,
    )
    return (final[0].T, final[1].T, final[2].T, final[3, :1, :ITERS])


def solution(mesh):
    sizes = (mesh.shape["region"], mesh.shape["feat"], mesh.shape["row"])
    return jax.shard_map(
        functools.partial(per_device, sizes),
        mesh=mesh,
        in_specs=(
            P(("region", "row"), None),
            P(("region", "row"), None),
            P(("region", "row")),
            P(None, "feat"),
            P("feat"),
            P(("region", "feat"), None),
            P(("region", "feat"), "row"),
            P(("region", "feat"), "row"),
            P("feat", "row"),
            P("region"),
        ),
        out_specs=(
            P(("region", "feat"), "row"),
            P(("region", "feat"), "row"),
            P("feat", "row"),
            P("region", None),
        ),
        check_vma=False,
    )
```

```python
import functools
import math

import jax
import jax.numpy as jnp
from jax import lax
from jax.experimental import pallas as pl
from jax.experimental.pallas import tpu as pltpu
from jax.sharding import PartitionSpec as P

ITERS = 3
CORES = 2
PARTS = 2
CHUNK = 2048
MESH = pl.DeviceIdType.MESH
INV_TURN = 1.0 / (2.0 * math.pi)
WAVE_GAIN, WAVE_MIDDLE, WAVE_LAST = 71.848585, -0.5703125, 0.08740234375
F32 = jnp.float32
BF16 = jnp.bfloat16


def dot(a, b):
    return lax.dot_general(a, b, (((1,), (0,)), ((), ())), preferred_element_type=F32)


def dot_nt(a, b):
    return lax.dot_general(a, b, (((1,), (1,)), ((), ())), preferred_element_type=F32)


def feature_tile(omega, phase, samples):
    turns = dot_nt(omega, samples) + phase
    rest = (0.25 - jnp.abs(turns - jnp.round(turns))).astype(BF16)
    square = rest * rest
    value = (square + jnp.asarray(WAVE_MIDDLE, BF16)) * square + jnp.asarray(WAVE_LAST, BF16)
    return value * rest


def invert(base, factor_ref, dinv_ref, n_ref, t_ref):
    size = factor_ref.shape[0]
    t_ref[...] = jnp.zeros_like(t_ref)
    powers, totals = [], []
    for start in range(0, size, base):
        rows = factor_ref[start : start + base, :]
        row = lax.broadcasted_iota(jnp.int32, rows.shape, 0) + start
        column = lax.broadcasted_iota(jnp.int32, rows.shape, 1)
        diagonal = jnp.sum(jnp.where(row == column, rows, 0.0), axis=1, keepdims=True)
        n_ref[start : start + base, :] = jnp.where(row > column, rows / diagonal, 0.0).astype(BF16)
        block = factor_ref[start : start + base, start : start + base]
        inner_row = lax.broadcasted_iota(jnp.int32, block.shape, 0)
        inner_column = lax.broadcasted_iota(jnp.int32, block.shape, 1)
        on = jnp.sum(jnp.where(inner_row == inner_column, block, 0.0), axis=0, keepdims=True)
        dinv_ref[:, start : start + base] = 1.0 / on
        power = -n_ref[start : start + base, start : start + base].astype(F32)
        powers.append(power)
        totals.append(power)
    reach = 2
    while reach < base:
        for index in range(len(powers)):
            low = powers[index].astype(BF16)
            square = dot(low, low)
            low = square.astype(BF16)
            totals[index] = totals[index] + square + dot(totals[index].astype(BF16), low)
            powers[index] = square
        reach *= 2
    for index, start in enumerate(range(0, size, base)):
        t_ref[start : start + base, start : start + base] = totals[index].astype(BF16)
    width = base
    while width < size:
        for start in range(0, size, 2 * width):
            top = slice(start, start + width)
            bottom = slice(start + width, start + 2 * width)
            below = n_ref[bottom, top]
            first = below.astype(F32) + dot(below, t_ref[top, top])
            second = first + dot(t_ref[bottom, bottom], first.astype(BF16))
            t_ref[bottom, top] = (-second).astype(BF16)
        width *= 2


def lower(rows, t_ref):
    size = t_ref.shape[0]
    step = min(256, size)
    pieces = [dot_nt(rows[:, : i + step], t_ref[i : i + step, : i + step]) for i in range(0, size, step)]
    return jnp.concatenate(pieces, axis=1)


def lower_flipped(rows, t_ref):
    size = t_ref.shape[0]
    step = min(256, size)
    pieces = [dot(rows[:, i:], t_ref[i:, i : i + step]) for i in range(0, size, step)]
    return jnp.concatenate(pieces, axis=1)


def admm_kernel(
    sizes,
    offset,
    scale,
    penalty_hbm,
    samples_hbm,
    targets_hbm,
    member_hbm,
    omega_hbm,
    phase_hbm,
    factor_hbm,
    weights_hbm,
    duals_hbm,
    consensus_hbm,
    out_hbm,
    factor_ref,
    dinv_ref,
    strict_ref,
    solve_ref,
    samples_ref,
    targets_ref,
    member_ref,
    omega_ref,
    phase_ref,
    state_ref,
    penalty_ref,
    feat_ref,
    flip_ref,
    coarse_ref,
    acc_ref,
    part_ref,
    other_ref,
    resid_ref,
    gfar_ref,
    gside_ref,
    gown_ref,
    gsend_ref,
    grow_ref,
    rs_send_ref,
    rs_recv_ref,
    mean_ref,
    gap_ref,
    load_sem,
    store_sem,
    omega_send,
    omega_recv,
    phase_send,
    phase_recv,
    crow_send,
    crow_recv,
    cside_send,
    cside_recv,
    core_send,
    core_recv,
    gside_send,
    gside_recv,
    grow_send,
    grow_recv,
    rs_send,
    rs_recv,
    mean_send,
    mean_recv,
    gap_send,
    gap_recv,
):
    n_region, n_feat, n_row = sizes
    narrow, width = weights_hbm.shape
    outputs = n_row * narrow
    lanes = width // 128
    inputs = omega_hbm.shape[0]
    gain = scale * WAVE_GAIN
    count = feat_ref.shape[2]
    chunk = min(CHUNK, count)
    chunks = count // chunk
    piece_width = width // PARTS
    tile = min(512, piece_width)
    small = tile // 2
    ratio, tiles, pieces = tile // small, width // tile, width // small
    region, feat, row = lax.axis_index("region"), lax.axis_index("feat"), lax.axis_index("row")
    group = n_feat * n_row
    place = feat * n_row + row
    side = (region, lax.rem(feat + CORES, n_feat), row)
    core = (region, feat + 1 - 2 * lax.rem(feat, CORES), row)

    def apart_rows(k):
        return min(k % n_row, n_row - k % n_row)

    def apart_regions(k):
        return min(k // CORES, n_region // CORES - k // CORES) + 2 * (k % CORES)

    def apart_group(k):
        return apart_rows(k) + 0.5 * min(k // n_row, n_feat - k // n_row)

    near_order = sorted(range(1, n_row), key=apart_rows, reverse=True)
    far_order = sorted(range(n_row), key=apart_rows, reverse=True)
    region_order = sorted(range(1, n_region), key=apart_regions, reverse=True)
    group_order = sorted(range(1, group), key=apart_group, reverse=True)

    def row_peer(k):
        return (region, feat, lax.rem(row + k, n_row))

    def region_peer(k):
        return (lax.rem(region + k, n_region), feat, row)

    def far_peer(k):
        return (region, lax.rem(feat + CORES, n_feat), lax.rem(row + k, n_row))

    def group_peer(k):
        other = lax.rem(place + k, group)
        return (region, other // n_row, lax.rem(other, n_row))

    def remote(src, dst, send, recv, device):
        return pltpu.make_async_remote_copy(
            src_ref=src, dst_ref=dst, send_sem=send, recv_sem=recv,
            device_id=device, device_id_type=MESH,
        )

    first = pl.multiple_of((feat // CORES) * count, 128)
    span = pl.ds(first, count)
    loads = [
        pltpu.make_async_copy(samples_hbm.at[span], samples_ref.at[:, :inputs], load_sem.at[0]),
        pltpu.make_async_copy(omega_hbm, omega_ref.at[0], load_sem.at[1]),
        pltpu.make_async_copy(phase_hbm, phase_ref.at[0], load_sem.at[2]),
        pltpu.make_async_copy(weights_hbm, state_ref.at[0], load_sem.at[3]),
        pltpu.make_async_copy(duals_hbm, state_ref.at[1], load_sem.at[4]),
        pltpu.make_async_copy(consensus_hbm, state_ref.at[2], load_sem.at[5]),
        pltpu.make_async_copy(penalty_hbm, penalty_ref, load_sem.at[9]),
        pltpu.make_async_copy(targets_hbm.at[:, span], targets_ref, load_sem.at[6]),
        pltpu.make_async_copy(member_hbm.at[:, span], member_ref, load_sem.at[7]),
        pltpu.make_async_copy(factor_hbm, factor_ref, load_sem.at[8]),
    ]
    for load in loads[:7]:
        load.start()

    barrier = pltpu.get_barrier_semaphore()
    for k in group_order:
        pl.semaphore_signal(barrier, inc=1, device_id=group_peer(k), device_id_type=MESH)
    for k in region_order:
        pl.semaphore_signal(barrier, inc=1, device_id=region_peer(k), device_id_type=MESH)

    def column_of(line):
        pieces = []
        for j in range(line.shape[1] // 128):
            level = lax.broadcasted_iota(jnp.int32, (128, 128), 0)
            across = lax.broadcasted_iota(jnp.int32, (128, 128), 1)
            only = jnp.where(level == across, line[:, 128 * j : 128 * (j + 1)], 0.0)
            pieces.append(jnp.sum(only, axis=1, keepdims=True))
        return jnp.concatenate(pieces, axis=0)

    def omega_piece(i):
        span = pl.ds(pl.multiple_of(i * small, small), small)
        return remote(
            omega_ref.at[0, :, span], omega_ref.at[1, :, span], omega_send.at[i], omega_recv.at[i],
            side,
        )

    def phase_copy():
        return remote(phase_ref.at[0], phase_ref.at[1], phase_send.at[0], phase_recv.at[0], side)

    def near_copies(t):
        mine = coarse_ref.at[t, 0, row]
        return [
            remote(mine, mine, crow_send.at[t], crow_recv.at[t], row_peer(k))
            for k in near_order
        ]

    def far_copies(t):
        mine, there = coarse_ref.at[t, 0, row], coarse_ref.at[t, 1, row]
        return [
            remote(mine, there, cside_send.at[t], cside_recv.at[t], far_peer(k))
            for k in far_order
        ]

    def arrived(pieces, semaphore):
        remote(pieces, pieces, semaphore, semaphore, side).wait_recv()

    def sent(pieces, semaphore):
        remote(pieces, pieces, semaphore, semaphore, side).wait_send()

    def core_copy(t, j):
        return remote(
            part_ref.at[t, j], other_ref.at[t, j], core_send.at[t, j], core_recv.at[t, j], core
        )

    def start(copies):
        for copy in copies:
            copy.start()

    def fill(half, down, size):
        rows = pl.ds(pl.multiple_of(down, size), size)
        part = (omega_ref[half, :, rows].astype(F32) * INV_TURN).T
        high = part.astype(BF16)
        low = (part - high.astype(F32)).astype(BF16)
        column = column_of(phase_ref[half, :, rows] * INV_TURN)
        both = jnp.concatenate([high, low], axis=1)
        value = feature_tile(both, column, samples_ref[...])
        feat_ref[half, rows, :] = value
        flip_ref[half, :, rows] = value.T

    def fill_small(i, carry):
        omega_piece(i).wait_recv()
        fill(1, i * small, small)
        return carry

    def fill_large(i, carry):
        @pl.when(i == 1)
        def _():
            pl.semaphore_wait(barrier, group - 1 + n_region - 1)
            start([phase_copy()])
            start([omega_piece(j) for j in range(pieces)])
            coarse_ref[0, 0, row] = state_ref[0].astype(BF16)
            start(near_copies(0))
            start(far_copies(0))

        @pl.when(i == tiles)
        def _():
            phase_copy().wait_recv()
            lax.fori_loop(0, ratio, fill_small, 0)

        @pl.when(i >= tiles)
        def _():
            for j in range(ratio):
                omega_piece(ratio * lax.rem(i + 1, tiles) + j).wait_recv()

        half = i // tiles
        fill(half, (i - half * (tiles - 1)) * tile, tile)
        return carry

    history = jnp.zeros((1, 128), F32)
    lane = lax.broadcasted_iota(jnp.int32, (1, 128), 1)
    with jax.named_scope("load0"):
        for load in loads[:7]:
            load.wait()
        for load in loads[7:]:
            load.start()
        samples_ref[:, inputs:] = samples_ref[:, :inputs]
    with jax.named_scope("fill"):
        lax.fori_loop(0, 2 * tiles - 1, fill_large, 0)
    weights, duals, consensus = state_ref[0], state_ref[1], state_ref[2]
    rho = jnp.broadcast_to(penalty_ref[...], (1, 128))

    for t in range(ITERS):
        with jax.named_scope("near_wait"):
            arrived(coarse_ref.at[t, 0, pl.ds(0, n_row - 1)], crow_recv.at[t])
        if t == 0:
            loads[7].wait()
            loads[8].wait()
        with jax.named_scope("pred_near"):
            near = coarse_ref[t, 0].reshape(outputs, width)
            for j in range(chunks):
                span = slice(j * chunk, (j + 1) * chunk)
                acc_ref[:, span] = dot(near, feat_ref[0, :, span])
        if t > 0:
            with jax.named_scope("share_mean"):
                share_mean(t - 1)
        with jax.named_scope("far_wait"):
            arrived(coarse_ref.at[t, 1], cside_recv.at[t])
        with jax.named_scope("pred_far"):
            far = coarse_ref[t, 1].reshape(outputs, width)
            for j in range(chunks):
                span = slice(j * chunk, (j + 1) * chunk)
                part = gain * (acc_ref[:, span] + dot(far, feat_ref[1, :, span]))
                acc_ref[:, span] = part
                part_ref[t, j] = part.astype(BF16)
                core_copy(t, j).start()
        with jax.named_scope("resid"):
            for j in range(chunks):
                span = slice(j * chunk, (j + 1) * chunk)
                core_copy(t, j).wait_recv()
                predicted = acc_ref[:, span] + other_ref[t, j].astype(F32)
                gap_value = predicted - targets_ref[:, span].astype(F32)
                resid_ref[:, span] = (member_ref[:, span].astype(F32) * gap_value).astype(BF16)

        with jax.named_scope("grad_far"):
            for p in range(PARTS):
                span = slice(p * piece_width, (p + 1) * piece_width)
                value = dot(resid_ref[...], flip_ref[1, :, span])
                gfar_ref[t, p] = value.astype(BF16).reshape(n_row, narrow, piece_width)
                for k in far_order:
                    target = lax.rem(row + k, n_row)
                    copy = remote(
                        gfar_ref.at[t, p, target], gside_ref.at[t, p, k], gside_send.at[t],
                        gside_recv.at[t], far_peer(k),
                    )
                    copy.start()
        with jax.named_scope("grad_near"):
            for p in range(PARTS):
                span = slice(p * piece_width, (p + 1) * piece_width)
                value = dot(resid_ref[...], flip_ref[0, :, span])
                value = value.reshape(n_row, narrow, piece_width)
                gown_ref[p] = value
                gsend_ref[t, p] = value.astype(BF16)
                for k in near_order:
                    target = lax.rem(row + k, n_row)
                    copy = remote(
                        gsend_ref.at[t, p, target], grow_ref.at[t, p, k], grow_send.at[t],
                        grow_recv.at[t], row_peer(k),
                    )
                    copy.start()
        if t == 0:
            with jax.named_scope("invert"):
                loads[9].wait()
                invert(min(256, width), factor_ref, dinv_ref, strict_ref, solve_ref)
        else:
            with jax.named_scope("finish_region"):
                apart, duals, consensus = finish_region(t - 1)
        dinv = dinv_ref[...]
        with jax.named_scope("grad_wait"):
            arrived(gside_ref.at[t], gside_recv.at[t])
            arrived(grow_ref.at[t, :, pl.ds(1, n_row - 1)], grow_recv.at[t])
            gradient = []
            for p in range(PARTS):
                value = gown_ref[p, row]
                for k in range(n_row):
                    value = value + gside_ref[t, p, k].astype(F32)
                for k in range(1, n_row):
                    value = value + grow_ref[t, p, k].astype(F32)
                gradient.append(value)
            gradient = gain * jnp.concatenate(gradient, axis=1)
        with jax.named_scope("solve"):
            scalar = rho[:, :1]
            if t == 0:
                right = gradient + scalar * (weights - consensus + duals)
            else:
                right = jnp.concatenate([gradient + scalar * duals, apart], axis=0)
            forward = right * dinv
            forward = forward + lower(forward.astype(BF16), solve_ref)
            update = (forward + lower_flipped(forward.astype(BF16), solve_ref)) * dinv
        if t > 0:
            with jax.named_scope("finish_gap"):
                rho, duals, history = finish_gap(t - 1, rho, duals, history)
            scalar = rho[:, :1]
            update = update[:narrow] + scalar * update[narrow:]
        weights = weights - update
        if t < ITERS - 1:
            coarse_ref[t + 1, 0, row] = weights.astype(BF16)
            start(near_copies(t + 1))

        total = scalar * (weights + duals)
        for c in range(n_region):
            down, right = 8 * (c // lanes), 128 * (c % lanes)
            rs_send_ref[t, c, :8] = total[down : down + 8, right : right + 128]
            rs_send_ref[t, c, 8:] = jnp.broadcast_to(scalar, (8, 128))
        rs_recv_ref[t, region] = rs_send_ref[t, region]
        for k in region_order:
            owner = lax.rem(region + k, n_region)
            copy = remote(
                rs_send_ref.at[t, owner, pl.ds(0, 9)], rs_recv_ref.at[t, region, pl.ds(0, 9)],
                rs_send.at[t], rs_recv.at[t], region_peer(k),
            )
            copy.start()
        if t < ITERS - 1:
            start(far_copies(t + 1))

        def share_mean(s):
            arrived(rs_recv_ref.at[s, pl.ds(0, n_region - 1), pl.ds(0, 9)], rs_recv.at[s])
            total = rs_recv_ref[s, 0, :9]
            for r in range(1, n_region):
                total = total + rs_recv_ref[s, r, :9]
            mean_ref[s, region] = (total[:8] / total[8:9]).astype(BF16)
            mine = mean_ref.at[s, region]
            for k in region_order:
                remote(mine, mine, mean_send.at[s], mean_recv.at[s], region_peer(k)).start()

        def finish_region(s, weights=weights, duals=duals, consensus=consensus):
            arrived(mean_ref.at[s, pl.ds(0, n_region - 1)], mean_recv.at[s])
            updated = jnp.concatenate(
                [
                    jnp.concatenate([mean_ref[s, h * lanes + j].astype(F32) for j in range(lanes)], axis=1)
                    for h in range(narrow // 8)
                ],
                axis=0,
            )
            gap = jnp.sum(jnp.square(weights - updated), keepdims=True).reshape(1, 1)
            drift = jnp.sum(jnp.square(updated - consensus), keepdims=True).reshape(1, 1)
            gap_ref[s, place, :1] = jnp.where(lane < 64, gap, drift)
            mine = gap_ref.at[s, place, pl.ds(0, 1)]
            for k in group_order:
                remote(mine, mine, gap_send.at[s], gap_recv.at[s], group_peer(k)).start()
            return weights - updated, duals + weights - updated, updated

        def finish_gap(s, rho, duals, history):
            arrived(gap_ref.at[s, pl.ds(0, group - 1), pl.ds(0, 1)], gap_recv.at[s])
            total = jnp.sum(gap_ref[s, :, :1], axis=0)
            gap = jnp.broadcast_to(total[:, :1], (1, 128))
            drift = jnp.broadcast_to(total[:, 64:65], (1, 128))
            drift = rho * rho * drift
            renewed = rho * jnp.sqrt((gap + offset) / (drift + offset))
            duals = duals * (rho / renewed)[:, :1]
            return renewed, duals, jnp.where(lane == s, renewed, history)

    def store(rows, value):
        state_ref[rows] = value
        copy = pltpu.make_async_copy(state_ref.at[rows], out_hbm.at[rows], store_sem.at[rows])
        copy.start()
        return copy

    stores = [store(0, weights)]
    with jax.named_scope("drain_early"):
        phase_copy().wait_send()
        for i in range(pieces):
            omega_piece(i).wait_send()
        for t in range(ITERS):
            sent(coarse_ref.at[t, 0, pl.ds(0, n_row - 1)], crow_send.at[t])
            sent(coarse_ref.at[t, 1], cside_send.at[t])
            for j in range(chunks):
                core_copy(t, j).wait_send()
            sent(gside_ref.at[t], gside_send.at[t])
            sent(grow_ref.at[t, :, pl.ds(1, n_row - 1)], grow_send.at[t])
            sent(rs_recv_ref.at[t, pl.ds(0, n_region - 1), pl.ds(0, 9)], rs_send.at[t])
            if t < ITERS - 1:
                sent(mean_ref.at[t, pl.ds(0, n_region - 1)], mean_send.at[t])
                sent(gap_ref.at[t, pl.ds(0, group - 1), pl.ds(0, 1)], gap_send.at[t])
    with jax.named_scope("last_mean"):
        share_mean(ITERS - 1)
    with jax.named_scope("last_region"):
        apart, duals, consensus = finish_region(ITERS - 1)
    stores.append(store(2, consensus))
    with jax.named_scope("last_gap"):
        rho, duals, history = finish_gap(ITERS - 1, rho, duals, history)
    stores.append(store(1, duals))
    stores.append(store(3, jnp.broadcast_to(jnp.tile(history, (1, width // 128)), (narrow, width))))
    with jax.named_scope("drain"):
        sent(mean_ref.at[ITERS - 1, pl.ds(0, n_region - 1)], mean_send.at[ITERS - 1])
        sent(gap_ref.at[ITERS - 1, pl.ds(0, group - 1), pl.ds(0, 1)], gap_send.at[ITERS - 1])
        for copy in stores:
            copy.wait()


def admm(sizes, offset, scale, penalty, samples, targets, member, omega, phase, factors, *state):
    n_region, n_feat, n_row = sizes
    narrow, width = state[0].shape
    outputs = n_row * narrow
    inputs = omega.shape[0]
    count = samples.shape[0] // (n_feat // CORES)
    chunk = min(CHUNK, count)
    chunks = count // chunk
    group = n_feat * n_row
    part = (n_row, narrow, width // PARTS)
    tiles = width // min(512, width // PARTS)
    hbm = pl.BlockSpec(memory_space=pl.ANY)
    dma = pltpu.SemaphoreType.DMA
    return pl.pallas_call(
        functools.partial(admm_kernel, sizes, offset, scale),
        in_specs=[hbm] * 10,
        out_specs=hbm,
        out_shape=jax.ShapeDtypeStruct((4, narrow, width), F32),
        scratch_shapes=[
            pltpu.VMEM((width, width), F32),
            pltpu.VMEM((1, width), F32),
            pltpu.VMEM((width, width), BF16),
            pltpu.VMEM((width, width), BF16),
            pltpu.VMEM((count, 2 * inputs), BF16),
            pltpu.VMEM((outputs, count), BF16),
            pltpu.VMEM((1, count), jnp.int32),
            pltpu.VMEM((2, inputs, width), BF16),
            pltpu.VMEM((2, 1, width), F32),
            pltpu.VMEM((4, narrow, width), F32),
            pltpu.VMEM((1, 1), F32),
            pltpu.VMEM((2, width, count), BF16),
            pltpu.VMEM((2, count, width), BF16),
            pltpu.VMEM((ITERS, 2, n_row, narrow, width), BF16),
            pltpu.VMEM((outputs, count), F32),
            pltpu.VMEM((ITERS, chunks, outputs, chunk), BF16),
            pltpu.VMEM((ITERS, chunks, outputs, chunk), BF16),
            pltpu.VMEM((outputs, count), BF16),
            pltpu.VMEM((ITERS, PARTS) + part, BF16),
            pltpu.VMEM((ITERS, PARTS) + part, BF16),
            pltpu.VMEM((PARTS,) + part, F32),
            pltpu.VMEM((ITERS, PARTS) + part, BF16),
            pltpu.VMEM((ITERS, PARTS) + part, BF16),
            pltpu.VMEM((ITERS, n_region, 16, 128), F32),
            pltpu.VMEM((ITERS, n_region, 16, 128), F32),
            pltpu.VMEM((ITERS, n_region, 8, 128), BF16),
            pltpu.VMEM((ITERS, group, 8, 128), F32),
            dma((10,)),
            dma((4,)),
            dma((2 * tiles,)),
            dma((2 * tiles,)),
            dma((1,)),
            dma((1,)),
            dma((ITERS,)),
            dma((ITERS,)),
            dma((ITERS,)),
            dma((ITERS,)),
            dma((ITERS, chunks)),
            dma((ITERS, chunks)),
            dma((ITERS,)),
            dma((ITERS,)),
            dma((ITERS,)),
            dma((ITERS,)),
            dma((ITERS,)),
            dma((ITERS,)),
            dma((ITERS,)),
            dma((ITERS,)),
            dma((ITERS,)),
            dma((ITERS,)),
        ],
        compiler_params=pltpu.CompilerParams(
            collective_id=0, has_side_effects=True, vmem_limit_bytes=63 * 2**20
        ),
        name="admm",
    )(penalty, samples, targets, member, omega, phase, factors, *state)


def per_device(
    sizes,
    samples,
    targets,
    member,
    omega,
    phase,
    factors,
    weights_init,
    duals_init,
    consensus_init,
    penalty_init,
):
    n_region, n_feat, n_row = sizes
    total_features = n_feat * omega.shape[1]
    total_outputs = targets.shape[1]
    offset = 0.01 * total_features * total_outputs
    scale = math.sqrt(2.0 / total_features)
    final = admm(
        sizes, offset, scale, penalty_init[None, :], samples, targets.T, member[None, :], omega,
        phase[None, :], factors, weights_init.T, duals_init.T, consensus_init.T,
    )
    return (final[0].T, final[1].T, final[2].T, final[3, :1, :ITERS])


def solution(mesh):
    sizes = (mesh.shape["region"], mesh.shape["feat"], mesh.shape["row"])
    return jax.shard_map(
        functools.partial(per_device, sizes),
        mesh=mesh,
        in_specs=(
            P(("region", "row"), None),
            P(("region", "row"), None),
            P(("region", "row")),
            P(None, "feat"),
            P("feat"),
            P(("region", "feat"), None),
            P(("region", "feat"), "row"),
            P(("region", "feat"), "row"),
            P("feat", "row"),
            P("region"),
        ),
        out_specs=(
            P(("region", "feat"), "row"),
            P(("region", "feat"), "row"),
            P("feat", "row"),
            P("region", None),
        ),
        check_vma=False,
    )
```
